32 devices in a mesh: dp: 8 (over y, x, core), mp: 4 (over z).
Axes of the slice: x: 2, y: 2, z: 4, core: 2. Of those that a mesh axis runs over, the one named last changes fastest.
Arguments:
- block_input: bfloat16 [192, 196, 512], P('dp'), may hold values from -6 to 6
- out_grad: bfloat16 [192, 196, 512], P('dp'), may hold values from -6 to 6
- norm_gains: bfloat16 [512, 2], P('dp'), may hold values from 0.5 to 1.5
- offsets: bfloat16 [512, 4], P('dp'), may hold values from -3 to 3
- qkv_weight: bfloat16 [512, 3, 512], P('dp', None, 'mp'), may hold values from -2 to 2
- qv_bias: bfloat16 [2, 512], P(None, 'mp'), may hold values from -3 to 3
- pos_table: float32 [16, 169], P('mp'), may hold values from -4 to 4
- proj_weight: bfloat16 [512, 512], P('dp', 'mp'), may hold values from -0.75 to 0.75
- fc1_weight: bfloat16 [512, 2048], P('dp', 'mp'), may hold values from -0.25 to 0.25
- fc1_bias: bfloat16 [2048], P('mp'), may hold values from -3 to 3
- fc2_weight: bfloat16 [512, 2048], P('dp', 'mp'), may hold values from -0.125 to 0.125
- rel_index: int32 [49, 49], replicated, may hold values from 0 to 168
- region_ids: int32 [14, 14], replicated, may hold values from 0 to 3
Outputs:
- block_output: bfloat16 [192, 196, 512], P('dp')
- input_grad: bfloat16 [192, 196, 512], P('dp')
- norm_gains_grad: float32 [512, 2], P('dp')
- offsets_grad: float32 [512, 4], P('dp')
- qkv_weight_grad: float32 [512, 3, 512], P('dp', None, 'mp')
- qv_bias_grad: float32 [2, 512], P(None, 'mp')
- pos_table_grad: float32 [16, 169], P('mp')
- proj_weight_grad: float32 [512, 512], P('dp', 'mp')
- fc1_weight_grad: float32 [512, 2048], P('dp', 'mp')
- fc1_bias_grad: float32 [2048], P('mp')
- fc2_weight_grad: float32 [512, 2048], P('dp', 'mp')
The draws below stay inside these ranges and needn't reach their ends.
All inputs are finite; a program needn't handle non-finite values.
Results may differ from the reference program's by a relative error of at most 0.04.
The reference program's roundings to bfloat16 on the way count: a program that leaves them out, or rounds other values in their place, can miss the bound.
Values may be sent and summed in bfloat16 or wider, within the bound.
A program may use at most 256 MiB of HBM per device.

```python
import math
import jax
import jax.numpy as jnp
from jax import lax

D = 512
HEADS = 16
FF = 2048
HD = 32
WIN = 7
SHIFT = 3
SIDE = 14
REGIONS = 4
TOK_IMG = 196
WPOS = 49
TABLE = 169
IMG_DEV = 24
IMAGES = 192
N_DP = 8
N_MP = 4


def draw_qkv_weight(key, part):
    key_base = jax.random.fold_in(key, 0)
    drawn = jax.random.normal(key_base, (D, 3, D), jnp.float32) * D ** (-0.5)
    return jnp.clip(drawn, -2.0, 2.0).astype(jnp.bfloat16)


def touch_ends(values, own_key, smallest, largest):
    spot = [jax.random.randint(jax.random.fold_in(own_key, axis), (), 0, length) for axis, length in enumerate(values.shape)]
    main_axis = values.shape.index(max(values.shape))
    neighbour = spot[:main_axis] + [(spot[main_axis] + 1) % values.shape[main_axis]] + spot[main_axis + 1:]
    return values.at[tuple(spot)].set(smallest).at[tuple(neighbour)].set(largest)


def shard_levels(rng, dims, shards, smallest, top_value):
    loudness = 1.0
    for axis_at, blocks in shards:
        steps = jax.random.uniform(jax.random.fold_in(jax.random.fold_in(rng, 6), axis_at), (blocks,), jnp.float32, smallest / len(shards), top_value / len(shards))
        loudness = loudness * jnp.repeat(jnp.exp(steps), dims[axis_at] // blocks).reshape((-1,) + (1,) * (len(dims) - 1 - axis_at))
    return loudness


def bell_draw(stream_key, dims, spread, most, cuts=(), kind=jnp.bfloat16):
    array = jax.random.normal(stream_key, dims, jnp.float32) * spread
    if len(cuts) > 0:
        array = shard_levels(stream_key, dims, cuts, -0.22, 0.18) * array
    return jnp.clip(array, min=-most, max=most).astype(kind)


def setup_inputs(seed: int = 0) -> dict:
    keys = jax.random.split(jax.random.key(seed), 14)
    block_input = bell_draw(keys[0], (IMAGES, TOK_IMG, D), 1.0, 6.0, ((0, 8),))
    out_grad = bell_draw(keys[1], (IMAGES, TOK_IMG, D), 1.0, 6.0, ((0, 8),))
    norm_gains = jnp.clip(1.0 + 0.1 * jax.random.normal(keys[2], (D, 2), jnp.float32), 0.5, 1.5).astype(jnp.bfloat16)
    offsets = bell_draw(keys[3], (D, 4), 0.5, 3.0, ((0, 8),))
    qkv_weight = draw_qkv_weight(jax.random.fold_in(keys[13], 71), 0)
    qv_bias = bell_draw(keys[5], (2, D), 0.5, 3.0, ((1, 4),))
    pos_table = bell_draw(keys[6], (HEADS, TABLE), 1.0, 4.0, ((0, 4),), jnp.float32)
    proj_weight = bell_draw(keys[7], (D, D), (D // 8) ** -0.5, 0.75, ((0, 8), (1, 4)))
    fc1_weight = bell_draw(keys[8], (D, FF), D ** -0.5, 0.25, ((0, 8), (1, 4)))
    fc1_bias = bell_draw(keys[9], (FF,), 0.5, 3.0, ((0, 4),))
    fc2_weight = bell_draw(keys[10], (D, FF), FF ** -0.5, 0.125, ((0, 8), (1, 4)))
    rel_index = touch_ends(jax.random.randint(keys[11], (WPOS, WPOS), 0, TABLE), jax.random.fold_in(keys[11], 1), 0, TABLE - 1).astype(jnp.int32)
    region_ids = touch_ends(jax.random.randint(keys[12], (SIDE, SIDE), 0, REGIONS), jax.random.fold_in(keys[12], 1), 0, REGIONS - 1).astype(jnp.int32)
    return {"block_input": block_input, "out_grad": out_grad, "norm_gains": norm_gains, "offsets": offsets, "qkv_weight": qkv_weight, "qv_bias": qv_bias, "pos_table": pos_table, "proj_weight": proj_weight, "fc1_weight": fc1_weight, "fc1_bias": fc1_bias, "fc2_weight": fc2_weight, "rel_index": rel_index, "region_ids": region_ids}


def rounded(array_in):
    return lax.optimization_barrier(array_in.astype(jnp.bfloat16)).astype(jnp.float32)

def window_order(tokens_in):
    image_count, channels = (tokens_in.shape[0], tokens_in.shape[-1])
    side_wins = SIDE // WIN
    grid_view = jnp.roll(tokens_in.reshape(image_count, SIDE, SIDE, channels), (-SHIFT, -SHIFT), axis=(1, 2))
    grid_view = grid_view.reshape(image_count, side_wins, WIN, side_wins, WIN, channels).transpose(0, 1, 3, 2, 4, 5)
    return grid_view.reshape(image_count, SIDE * SIDE, channels)

def grid_order(tokens_in):
    image_count, channels = (tokens_in.shape[0], tokens_in.shape[-1])
    side_wins = SIDE // WIN
    grid_view = tokens_in.reshape(image_count, side_wins, side_wins, WIN, WIN, channels).transpose(0, 1, 3, 2, 4, 5)
    grid_view = jnp.roll(grid_view.reshape(image_count, SIDE, SIDE, channels), (SHIFT, SHIFT), axis=(1, 2))
    return grid_view.reshape(image_count, SIDE * SIDE, channels)

def layer_norm(values, gain_col, shift_col):
    row_mean = lax.optimization_barrier(jnp.mean(values, axis=-1, keepdims=True))
    centred = values - row_mean
    variance = lax.optimization_barrier(jnp.mean(centred * centred, axis=-1, keepdims=True))
    inv_std = lax.rsqrt(variance + 1e-05)
    normed = centred * inv_std
    return (normed, inv_std, normed * gain_col + shift_col)

def norm_back(grad_out, normed, inv_std, gain_col):
    scaled = grad_out * gain_col
    return inv_std * (scaled - lax.optimization_barrier(jnp.mean(scaled, axis=-1, keepdims=True)) - normed * lax.optimization_barrier(jnp.mean(scaled * normed, axis=-1, keepdims=True)))

def gelu_parts(pre_act):
    cdf_val = 0.5 * (1.0 + jax.scipy.special.erf(pre_act * (1.0 / math.sqrt(2.0))))
    density = jnp.exp(-0.5 * pre_act * pre_act) * (1.0 / math.sqrt(2.0 * math.pi))
    return (pre_act * cdf_val, cdf_val + pre_act * density)

def window_terms(table_rows, rel_index, region_ids, block_size):
    table_len = table_rows.shape[1]
    win_pos = rel_index.shape[0]
    one_hot = (rel_index.reshape(-1)[:, None] == jnp.arange(table_len, dtype=jnp.int32)[None, :]).astype(jnp.float32)
    pos_bias = jnp.dot(table_rows.astype(jnp.float32), one_hot.T, precision=lax.Precision.HIGHEST).reshape(-1, win_pos, win_pos)
    side_wins = SIDE // WIN
    labels = region_ids.reshape(side_wins, WIN, side_wins, WIN).transpose(0, 2, 1, 3).reshape(side_wins * side_wins, win_pos)
    penalty = jnp.where(labels[:, :, None] == labels[:, None, :], 0.0, -100.0).astype(jnp.float32)
    win_bias = pos_bias[None] + penalty[:, None]
    return (jnp.tile(win_bias, (block_size, 1, 1, 1)), one_hot)

def blocked(image_count):
    for block_size in range(12, 0, -1):
        if image_count % block_size == 0:
            return block_size
    return 1

def attend(queries, key_rows, values, win_bias):
    scores = jnp.einsum('bqhc,bkhc->bhqk', queries, key_rows) + win_bias
    row_max = lax.optimization_barrier(jnp.max(scores, axis=-1, keepdims=True))
    weights_raw = jnp.exp(scores - row_max)
    row_total = lax.optimization_barrier(jnp.sum(weights_raw, axis=-1, keepdims=True))
    probs = rounded(weights_raw / row_total)
    attn_rows = rounded(jnp.einsum('bhqk,bkhc->bqhc', probs, values))
    return (attn_rows, (row_max + jnp.log(row_total))[..., 0])

def attend_back(queries, key_rows, values, attn_rows, grad_attn, log_total, win_bias):
    scores = jnp.einsum('bqhc,bkhc->bhqk', queries, key_rows) + win_bias
    probs = jnp.exp(scores - log_total[..., None])
    grad_probs = jnp.einsum('bqhc,bkhc->bhqk', grad_attn, values)
    delta = lax.optimization_barrier(jnp.sum(grad_attn * attn_rows, axis=-1)).transpose(0, 2, 1)
    grad_scores = probs * (grad_probs - delta[..., None])
    grad_sb = rounded(grad_scores)
    grad_q = jnp.einsum('bhqk,bkhc->bqhc', grad_sb, key_rows) * HD ** (-0.5)
    grad_k = jnp.einsum('bhqk,bqhc->bkhc', grad_sb, queries)
    grad_v = jnp.einsum('bhqk,bqhc->bkhc', rounded(probs), grad_attn)
    table_part = lax.optimization_barrier(jnp.sum(grad_scores, axis=0))
    return (grad_q, grad_k, grad_v, table_part)

def group_sum(left_part, right_part, spec_text):
    partial_value = jnp.einsum(spec_text, left_part.astype(jnp.float32), right_part.astype(jnp.float32))
    return lax.optimization_barrier(jnp.sum(rounded(partial_value), axis=1))

def reference(block_input, out_grad, norm_gains, offsets, qkv_weight, qv_bias, pos_table, proj_weight, fc1_weight, fc1_bias, fc2_weight, rel_index, region_ids):
    gain_cols = norm_gains.astype(jnp.float32)
    offset_cols = offsets.astype(jnp.float32)
    bias_qv = qv_bias.astype(jnp.float32)
    bias_hidden = fc1_bias.astype(jnp.float32)
    score_scale = HD ** (-0.5)
    head_cols = D // N_MP
    hidden_cols = FF // N_MP
    row_count = IMG_DEV * TOK_IMG
    block_size = blocked(IMG_DEV)
    block_count = IMG_DEV // block_size
    win_pos = rel_index.shape[0]
    win_count = TOK_IMG // win_pos
    win_bias, one_hot = window_terms(pos_table, rel_index, region_ids, block_size)

    def split_heads(flat_rows):
        return flat_rows.reshape(block_count, block_size * win_count, win_pos, HEADS, HD)

    def forward_block(operands):
        return attend(operands[0], operands[1], operands[2], win_bias)

    def backward_block(operands):
        return attend_back(operands[0], operands[1], operands[2], operands[3], operands[4], operands[5], win_bias)

    def group_step(totals, group_pair):
        images, cotangent = group_pair
        x_zero = window_order(images.astype(jnp.float32)).reshape(row_count, D)
        normed1, inv_std1, pre_one = layer_norm(x_zero, gain_cols[:, 0], offset_cols[:, 0])
        h_one = pre_one.astype(jnp.bfloat16)
        qkv_all = jnp.dot(h_one, qkv_weight.reshape(D, 3 * D), preferred_element_type=jnp.float32).reshape(row_count, 3, D)
        queries = rounded((qkv_all[:, 0] + bias_qv[0]) * score_scale)
        key_rows = rounded(qkv_all[:, 1])
        values = rounded(qkv_all[:, 2] + bias_qv[1])
        attn_rows, log_total = lax.map(forward_block, (split_heads(queries), split_heads(key_rows), split_heads(values)))
        attn_flat = attn_rows.reshape(row_count, D)
        attn_out = group_sum(attn_flat.reshape(row_count, N_MP, head_cols), proj_weight.reshape(D, N_MP, head_cols), 'rgf,dgf->rgd') + offset_cols[:, 1]
        x_one = x_zero + attn_out
        normed2, inv_std2, pre_two = layer_norm(x_one, gain_cols[:, 1], offset_cols[:, 2])
        h_two = pre_two.astype(jnp.bfloat16)
        pre_act = jnp.dot(h_two, fc1_weight, preferred_element_type=jnp.float32) + bias_hidden
        act_val, act_slope = gelu_parts(pre_act)
        act_rows = act_val.astype(jnp.bfloat16)
        mlp_out = group_sum(act_rows.reshape(row_count, N_MP, hidden_cols), fc2_weight.reshape(D, N_MP, hidden_cols), 'rgf,dgf->rgd') + offset_cols[:, 3]
        output = grid_order((x_one + mlp_out).reshape(IMG_DEV, TOK_IMG, D)).astype(jnp.bfloat16)
        grad_y = window_order(cotangent).reshape(row_count, D)
        grad_yf = grad_y.astype(jnp.float32)
        grad_fc2b = lax.optimization_barrier(jnp.sum(grad_yf, axis=0))
        grad_fc2 = jnp.dot(grad_y.T, act_rows, preferred_element_type=jnp.float32)
        grad_act = jnp.dot(grad_y, fc2_weight, preferred_element_type=jnp.float32)
        grad_pre = grad_act * act_slope
        grad_preb = grad_pre.astype(jnp.bfloat16)
        grad_fc1 = jnp.dot(h_two.T, grad_preb, preferred_element_type=jnp.float32)
        grad_fc1b = lax.optimization_barrier(jnp.sum(grad_pre, axis=0))
        grad_h2 = group_sum(grad_preb.reshape(row_count, N_MP, hidden_cols), fc1_weight.reshape(D, N_MP, hidden_cols), 'rgf,dgf->rgd')
        grad_ln2 = lax.optimization_barrier(jnp.sum(grad_h2 * normed2, axis=0))
        grad_ln2b = lax.optimization_barrier(jnp.sum(grad_h2, axis=0))
        grad_x1 = grad_yf + norm_back(grad_h2, normed2, inv_std2, gain_cols[:, 1])
        grad_x1b = grad_x1.astype(jnp.bfloat16)
        grad_proj = jnp.dot(grad_x1b.T, attn_flat.astype(jnp.bfloat16), preferred_element_type=jnp.float32)
        grad_projb = lax.optimization_barrier(jnp.sum(grad_x1, axis=0))
        grad_attn = rounded(jnp.dot(grad_x1b, proj_weight, preferred_element_type=jnp.float32))
        grad_q, grad_k, grad_v, table_part = lax.map(backward_block, (split_heads(queries), split_heads(key_rows), split_heads(values), split_heads(attn_flat), split_heads(grad_attn), log_total))
        grad_q = grad_q.reshape(row_count, D)
        grad_k = grad_k.reshape(row_count, D)
        grad_v = grad_v.reshape(row_count, D)
        grad_qv = jnp.stack([lax.optimization_barrier(jnp.sum(grad_q, axis=0)), lax.optimization_barrier(jnp.sum(grad_v, axis=0))])
        grad_qkv = rounded(jnp.stack([grad_q, grad_k, grad_v], axis=1))
        grad_qkvw = jnp.einsum('rd,rjc->djc', rounded(pre_one), grad_qkv)
        grad_h1 = group_sum(grad_qkv.reshape(row_count, 3, N_MP, head_cols), qkv_weight.reshape(D, 3, N_MP, head_cols), 'rjgc,djgc->rgd')
        grad_ln1 = lax.optimization_barrier(jnp.sum(grad_h1 * normed1, axis=0))
        grad_ln1b = lax.optimization_barrier(jnp.sum(grad_h1, axis=0))
        grad_x0 = grad_x1 + norm_back(grad_h1, normed1, inv_std1, gain_cols[:, 0])
        grad_in = grid_order(grad_x0.reshape(IMG_DEV, TOK_IMG, D)).astype(jnp.bfloat16)
        group_terms = (jnp.stack([grad_ln1, grad_ln2], axis=1), jnp.stack([grad_ln1b, grad_projb, grad_ln2b, grad_fc2b], axis=1), grad_qkvw, grad_qv, lax.optimization_barrier(jnp.sum(table_part, axis=0)), grad_proj, grad_fc1, grad_fc1b, grad_fc2)
        totals = jax.tree.map(jnp.add, totals, group_terms)
        return (totals, (output, grad_in))
    zeros_init = (jnp.zeros((D, 2), jnp.float32), jnp.zeros((D, 4), jnp.float32), jnp.zeros((D, 3, D), jnp.float32), jnp.zeros((2, D), jnp.float32), jnp.zeros((HEADS, win_pos, win_pos), jnp.float32), jnp.zeros((D, D), jnp.float32), jnp.zeros((D, FF), jnp.float32), jnp.zeros((FF,), jnp.float32), jnp.zeros((D, FF), jnp.float32))
    stacked = (block_input.reshape(N_DP, IMG_DEV, TOK_IMG, D), out_grad.reshape(N_DP, IMG_DEV, TOK_IMG, D))
    totals, group_outs = lax.scan(group_step, zeros_init, stacked)
    table_grad = jnp.dot(totals[4].reshape(HEADS, -1), one_hot, precision=lax.Precision.HIGHEST)
    return (group_outs[0].reshape(IMAGES, TOK_IMG, D), group_outs[1].reshape(IMAGES, TOK_IMG, D), totals[0], totals[1], totals[2], totals[3], table_grad, totals[5], totals[6], totals[7], totals[8])
```

```python
import functools
import math

import jax
import jax.numpy as jnp
import numpy as np
from jax import lax
from jax.experimental import pallas as pl
from jax.experimental.pallas import tpu as pltpu
from jax.sharding import PartitionSpec as P

HD = 32
WIN = 7
SHIFT = 3
SIDE = 14
F32 = jnp.float32
BF16 = jnp.bfloat16
WPAD = 64
EPS = 1e-05
DEAD = -1e30


def dot(a, b, ca=1, cb=0):
    return lax.dot_general(a, b, (((ca,), (cb,)), ((), ())), preferred_element_type=F32)


def padded_order():
    sides = SIDE // WIN
    wpos = WIN * WIN
    rows = np.full((sides * sides * WPAD,), -1, np.int32)
    for wr in range(sides):
        for wc in range(sides):
            for a in range(wpos):
                r = (wr * WIN + a // WIN + SHIFT) % SIDE
                c = (wc * WIN + a % WIN + SHIFT) % SIDE
                rows[(wr * sides + wc) * WPAD + a] = r * SIDE + c
    return rows


def pick_matrix(tokens):
    rows = padded_order()
    return (rows[:, None] == np.arange(tokens)[None, :]).astype(np.float32)


def norm(x):
    mean = jnp.mean(x, axis=-1, keepdims=True)
    cen = x - mean
    var = jnp.mean(cen * cen, axis=-1, keepdims=True)
    inv = lax.rsqrt(var + EPS)
    return cen * inv, inv


def norm_back(grad, normed, inv, gain):
    scaled = grad * gain
    return inv * (
        scaled
        - jnp.mean(scaled, axis=-1, keepdims=True)
        - normed * jnp.mean(scaled * normed, axis=-1, keepdims=True)
    )


def col_sum(v):
    return jnp.sum(v, axis=0, keepdims=True)


def head_masks(group_heads):
    lane_q = lax.broadcasted_iota(jnp.int32, (group_heads * WPAD, group_heads * HD), 0)
    lane_c = lax.broadcasted_iota(jnp.int32, (group_heads * WPAD, group_heads * HD), 1)
    return (lane_q // WPAD) == (lane_c // HD)


def spread(rows, mask, group_heads):
    tiled = jnp.concatenate([rows] * group_heads, axis=0)
    return jnp.where(mask, tiled, jnp.zeros_like(tiled))


def gather_heads(full, mask, group_heads):
    kept = jnp.where(mask, full, 0.0)
    total = kept[0:WPAD]
    for h in range(1, group_heads):
        total = total + kept[h * WPAD : (h + 1) * WPAD]
    return total


def attention_kernel(
    off_ref, x_ref, w_ref, vec_ref, qvb_ref, bias_ref, pm_ref, pmt_ref,
    qkv_ref, hw_ref, probs_ref, attn_ref, attw, *, imgs, groups, gh, prow, trow,
):
    gc = gh * HD
    full = groups * gc
    gain = vec_ref[0:1, :]
    shift = vec_ref[2:3, :]
    for im in range(imgs):
        normed, _ = norm(x_ref[im].astype(F32))
        h1 = (normed * gain + shift).astype(BF16)
        hw_ref[im * prow : (im + 1) * prow, :] = dot(pm_ref[...], h1).astype(BF16)
    hw = hw_ref[...]
    for kind in range(3):
        wk = jnp.concatenate([w_ref[g, :, kind * gc : (kind + 1) * gc] for g in range(groups)], axis=1)
        part = dot(hw, wk)
        if kind == 0:
            part = (part + qvb_ref[0:1, :]) * (HD**-0.5)
        if kind == 2:
            part = part + qvb_ref[1:2, :]
        qkv_ref[:, kind * full : (kind + 1) * full] = part.astype(BF16)
    wins = prow // WPAD
    mask = head_masks(gh)

    def window(i, carry):
        rows = pl.ds(pl.multiple_of(i * WPAD, WPAD), WPAD)
        win = lax.rem(i, wins)
        for g in range(groups):
            q = qkv_ref[rows, g * gc : (g + 1) * gc]
            k = qkv_ref[rows, full + g * gc : full + (g + 1) * gc]
            v = qkv_ref[rows, 2 * full + g * gc : 2 * full + (g + 1) * gc]
            scores = dot(k, spread(q, mask, gh), 1, 1) + bias_ref[g, win]
            e = jnp.exp(scores - jnp.max(scores, axis=0, keepdims=True))
            p = e * (1.0 / jnp.sum(e, axis=0, keepdims=True))
            probs_ref[i, g] = p
            o = gather_heads(dot(p.astype(BF16), v, 0, 0), mask, gh)
            attw[rows, g * gc : (g + 1) * gc] = o.astype(BF16)
        return carry

    lax.fori_loop(0, imgs * wins, window, 0)
    for im in range(imgs):
        attn_ref[im * trow : (im + 1) * trow, :] = dot(
            pmt_ref[...], attw[im * prow : (im + 1) * prow, :]
        ).astype(BF16)


def gelu_parts(pre):
    cdf = 0.5 * (1.0 + lax.erf(pre * (1.0 / math.sqrt(2.0))))
    density = jnp.exp(-0.5 * pre * pre) * (1.0 / math.sqrt(2.0 * math.pi))
    return pre * cdf, cdf + pre * density


def feed_kernel(
    off_ref, x_ref, gy_ref, attn_ref, w_ref, vec_ref, hb_ref,
    out_ref, gx1_ref, gw_ref, gb_ref, sums_ref,
    xs, gys, h2s, gyt, h2t, mlp, gh2, acc_p, acc_1, acc_2, *, imgs, groups, gc, trow, tokens,
):
    step = pl.program_id(0)
    d = vec_ref.shape[1]
    hid = hb_ref.shape[2]

    @pl.when(step == 0)
    def _():
        acc_p[...] = jnp.zeros_like(acc_p)
        acc_1[...] = jnp.zeros_like(acc_1)
        acc_2[...] = jnp.zeros_like(acc_2)
        gb_ref[...] = jnp.zeros_like(gb_ref)
        sums_ref[...] = jnp.zeros_like(sums_ref)
        xs[...] = jnp.zeros_like(xs)
        gys[...] = jnp.zeros_like(gys)

    for im in range(imgs):
        xs[im * trow : im * trow + tokens, :] = x_ref[im].astype(F32)
        gys[im * trow : im * trow + tokens, :] = gy_ref[im].astype(F32)
    proj = jnp.concatenate([w_ref[g, :, 0:gc] for g in range(groups)], axis=1)
    attn = attn_ref[...]
    x1 = xs[...] + dot(attn, proj, 1, 1) + vec_ref[3:4, :]
    xs[...] = x1
    normed2, inv2 = norm(x1)
    h2f = normed2 * vec_ref[1:2, :] + vec_ref[4:5, :]
    h2s[...] = h2f.astype(BF16)
    h2t[...] = h2f.T.astype(BF16)
    gyt[...] = gys[...].T.astype(BF16)
    mlp[...] = jnp.zeros_like(mlp)
    gh2[...] = jnp.zeros_like(gh2)

    def group(g, carry):
        fc1 = w_ref[g, :, gc : gc + hid]
        fc2 = w_ref[g, :, gc + hid : gc + 2 * hid]
        pre = dot(h2s[...], fc1) + hb_ref[g]
        act, slope = gelu_parts(pre)
        act = act.astype(BF16)
        gpre = dot(gys[...].astype(BF16), fc2) * slope
        gpb = gpre.astype(BF16)
        gb_ref[g] += col_sum(gpre)
        mlp[...] += dot(act, fc2, 1, 1)
        acc_2[g] += dot(gyt[...], act)
        gh2[...] += dot(gpb, fc1, 1, 1)
        acc_1[g] += dot(h2t[...], gpb)
        return carry

    lax.fori_loop(0, groups, group, 0)
    out = xs[...] + mlp[...] + vec_ref[5:6, :]
    for im in range(imgs):
        out_ref[im] = out[im * trow : im * trow + tokens].astype(BF16)
    normed2, inv2 = norm(xs[...])
    grad = gh2[...]
    gy = gys[...]
    gx1 = gy + norm_back(grad, normed2, inv2, vec_ref[1:2, :])
    gx1_ref[...] = gx1
    gx1b = gx1.astype(BF16)
    acc_p[...] += dot(gx1.T.astype(BF16), attn)
    sums_ref[0:1, :] += col_sum(grad * normed2)
    sums_ref[1:2, :] += col_sum(gx1)
    sums_ref[2:3, :] += col_sum(grad)
    sums_ref[3:4, :] += col_sum(gy)

    @pl.when(step == pl.num_programs(0) - 1)
    def _():
        for g in range(groups):
            gw_ref[g, :, 0:gc] = acc_p[:, g * gc : (g + 1) * gc].astype(BF16)
            gw_ref[g, :, gc : gc + hid] = acc_1[g].astype(BF16)
            gw_ref[g, :, gc + hid : gc + 2 * hid] = acc_2[g].astype(BF16)


def attention_back_kernel(
    off_ref, x_ref, gx1_ref, qkv_ref, hw_ref, probs_ref, wa_ref, wp_ref, vec_ref, pm_ref, pmt_ref,
    gin_ref, gw_ref, table_ref, qvs_ref, sums_ref,
    gxw, ga, gqkv, hwt, acc, *, imgs, groups, gh, prow, trow, tokens,
):
    step = pl.program_id(0)
    gc = gh * HD
    full = groups * gc

    @pl.when(step == 0)
    def _():
        acc[...] = jnp.zeros_like(acc)
        table_ref[...] = jnp.zeros_like(table_ref)
        qvs_ref[...] = jnp.zeros_like(qvs_ref)
        sums_ref[...] = jnp.zeros_like(sums_ref)

    for im in range(imgs):
        gxw[im * prow : (im + 1) * prow, :] = dot(
            pm_ref[...], gx1_ref[im * trow : (im + 1) * trow, :].astype(BF16)
        ).astype(BF16)
    proj = jnp.concatenate([wp_ref[g, :, 0:gc] for g in range(groups)], axis=1)
    ga[...] = dot(gxw[...], proj).astype(BF16)
    hwt[...] = hw_ref[...].astype(F32).T.astype(BF16)
    mask = head_masks(gh)
    wins = prow // WPAD

    def window(i, carry):
        rows = pl.ds(pl.multiple_of(i * WPAD, WPAD), WPAD)
        for g in range(groups):
            cols = slice(g * gc, (g + 1) * gc)
            q = qkv_ref[rows, g * gc : (g + 1) * gc]
            k = qkv_ref[rows, full + g * gc : full + (g + 1) * gc]
            v = qkv_ref[rows, 2 * full + g * gc : 2 * full + (g + 1) * gc]
            p = probs_ref[i, g]
            gas = spread(ga[rows, cols], mask, gh)
            dp = dot(v, gas, 1, 1)
            ds = p * (dp - jnp.sum(p * dp, axis=0, keepdims=True))
            table_ref[g] += ds
            dsb = ds.astype(BF16)
            gq = gather_heads(dot(dsb, k, 0, 0), mask, gh) * (HD**-0.5)
            gk = dot(dsb, spread(q, mask, gh))
            gv = dot(p.astype(BF16), gas)
            qvs_ref[0:1, cols] += col_sum(gq)
            qvs_ref[1:2, cols] += col_sum(gv)
            gqkv[rows, g * gc : (g + 1) * gc] = gq.astype(BF16)
            gqkv[rows, full + g * gc : full + (g + 1) * gc] = gk.astype(BF16)
            gqkv[rows, 2 * full + g * gc : 2 * full + (g + 1) * gc] = gv.astype(BF16)
        return carry

    lax.fori_loop(0, imgs * wins, window, 0)
    gh1 = None
    for kind in range(3):
        wk = jnp.concatenate([wa_ref[g, :, kind * gc : (kind + 1) * gc] for g in range(groups)], axis=1)
        part = gqkv[:, kind * full : (kind + 1) * full]
        term = dot(part, wk, 1, 1)
        gh1 = term if gh1 is None else gh1 + term
        acc[kind] += dot(hwt[...], part)
    gh1b = gh1.astype(BF16)
    for im in range(imgs):
        grad = dot(pmt_ref[...], gh1b[im * prow : (im + 1) * prow])[0:tokens]
        normed, inv = norm(x_ref[im].astype(F32))
        sums_ref[0:1, :] += col_sum(grad * normed)
        sums_ref[1:2, :] += col_sum(grad)
        gx0 = gx1_ref[im * trow : im * trow + tokens, :] + norm_back(grad, normed, inv, vec_ref[0:1, :])
        gin_ref[im] = gx0.astype(BF16)

    @pl.when(step == pl.num_programs(0) - 1)
    def _():
        for g in range(groups):
            for kind in range(3):
                gw_ref[g, :, kind * gc : (kind + 1) * gc] = acc[kind, :, g * gc : (g + 1) * gc].astype(BF16)


def whole(shape):
    zero = (0,) * len(shape)
    return pl.BlockSpec(shape, lambda i, off: zero, pipeline_mode=pl.Buffered(1))


def split3(v):
    hi = lax.reduce_precision(v, 8, 7)
    mid = lax.reduce_precision(v - hi, 8, 7)
    lo = v - hi - mid
    return [hi, mid, lo]


def shards(
    block_input, out_grad, norm_gains, offsets, qkv_weight, qv_bias, pos_table,
    proj_weight, fc1_weight, fc1_bias, fc2_weight, rel_index, region_ids, *, n_dp, n_mp,
):
    images, tokens, d = block_input.shape
    groups = n_mp
    gh, table_len = pos_table.shape
    gc = gh * HD
    hid = fc1_bias.shape[0]
    heads = groups * gh
    rows_w = qkv_weight.shape[0]
    wpos = rel_index.shape[0]
    wins = tokens // wpos
    prow = wins * WPAD
    trow = -(-tokens // 16) * 16
    mine = images // n_mp
    imgs = 2 if mine % 2 == 0 else 1
    steps = mine // imgs
    off = (lax.axis_index("mp") * steps).astype(jnp.int32).reshape(1)

    small = jnp.concatenate(
        [qv_bias.reshape(-1), fc1_bias] + [p.reshape(-1).astype(BF16) for p in split3(pos_table)]
    )
    per_row = -(-small.shape[0] // rows_w)
    small = jnp.pad(small, (0, per_row * rows_w - small.shape[0])).reshape(rows_w, per_row)
    n_vec = norm_gains.shape[1] + offsets.shape[1]
    extra = -(-(per_row + n_vec) // 128) * 128
    pack_a = jnp.concatenate(
        [
            qkv_weight.reshape(rows_w, 3 * gc), norm_gains, offsets, small,
            jnp.zeros((rows_w, extra - per_row - n_vec), BF16),
        ],
        axis=1,
    )
    pack_b = jnp.concatenate([proj_weight, fc1_weight, fc2_weight], axis=1)

    def gather(pack):
        got = lax.all_gather(lax.all_gather(pack, "mp", axis=0, tiled=False), "dp", axis=1, tiled=True)
        return got

    wa = gather(pack_a)
    wb = gather(pack_b)
    vec = jnp.pad(wa[0, :, 3 * gc : 3 * gc + n_vec].astype(F32).T, ((0, 2), (0, 0)))
    small = wa[:, 0:rows_w, 3 * gc + n_vec : 3 * gc + n_vec + per_row].reshape(groups, -1).astype(F32)
    qvb = small[:, 0 : 2 * gc].reshape(groups, 2, gc).transpose(1, 0, 2).reshape(2, groups * gc)
    qvb = jnp.pad(qvb, ((0, 6), (0, 0)))
    hb = small[:, 2 * gc : 2 * gc + hid].reshape(groups, 1, hid)
    tab = small[:, 2 * gc + hid : 2 * gc + hid + 3 * gh * table_len].reshape(groups, 3, gh, table_len)
    table = (tab[:, 0] + tab[:, 1] + tab[:, 2]).reshape(heads, table_len)

    pad_w = WPAD - wpos
    rel_t = jnp.pad(rel_index.T, ((0, pad_w), (0, pad_w)), constant_values=-1)
    one_hot = (rel_t.reshape(-1)[None, :] == jnp.arange(table_len, dtype=jnp.int32)[:, None]).astype(F32)
    pos = jnp.dot(table, one_hot, precision=lax.Precision.HIGHEST).reshape(groups, gh, WPAD, WPAD)
    side_wins = SIDE // WIN
    labels = (
        region_ids.reshape(side_wins, WIN, side_wins, WIN).transpose(0, 2, 1, 3).reshape(wins, wpos)
    )
    pen = jnp.where(labels[:, :, None] == labels[:, None, :], 0.0, -100.0).astype(F32)
    pen = jnp.pad(pen, ((0, 0), (0, 0), (0, pad_w)))
    pen = jnp.pad(pen, ((0, 0), (0, pad_w), (0, 0)), constant_values=DEAD)
    bias = pos.transpose(0, 2, 1, 3)[:, None] + pen[None, :, :, None, :]
    bias = bias.reshape(groups, wins, WPAD, gh * WPAD)

    pick = pick_matrix(tokens)
    pick_pad = np.pad(pick, ((0, 0), (0, trow - tokens)))
    pm = jnp.asarray(pick, BF16)
    pmp = jnp.asarray(pick_pad, BF16)
    pmt = jnp.asarray(pick_pad.T, BF16)
    params = pltpu.CompilerParams(vmem_limit_bytes=60 * 1024 * 1024)
    img_spec = pl.BlockSpec((imgs, tokens, d), lambda i, o: (o[0] + i, 0, 0))
    out_img_spec = pl.BlockSpec((imgs, tokens, d), lambda i, o: (i, 0, 0))
    full = groups * gc

    def rows_spec(r, c):
        return pl.BlockSpec((r, c), lambda i, o: (i, 0))

    probs_spec = pl.BlockSpec((imgs * wins, groups, WPAD, gh * WPAD), lambda i, o: (i, 0, 0, 0))
    qkv, hw, probs, attn = pl.pallas_call(
        functools.partial(attention_kernel, imgs=imgs, groups=groups, gh=gh, prow=prow, trow=trow),
        out_shape=(
            jax.ShapeDtypeStruct((mine * prow, 3 * full), BF16),
            jax.ShapeDtypeStruct((mine * prow, d), BF16),
            jax.ShapeDtypeStruct((mine * wins, groups, WPAD, gh * WPAD), F32),
            jax.ShapeDtypeStruct((mine * trow, full), BF16),
        ),
        grid_spec=pltpu.PrefetchScalarGridSpec(
            num_scalar_prefetch=1,
            grid=(steps,),
            in_specs=[
                img_spec, whole(wa.shape), whole(vec.shape), whole(qvb.shape), whole(bias.shape),
                whole(pm.shape), whole(pmt.shape),
            ],
            out_specs=[
                rows_spec(imgs * prow, 3 * full), rows_spec(imgs * prow, d), probs_spec,
                rows_spec(imgs * trow, full),
            ],
            scratch_shapes=[pltpu.VMEM((imgs * prow, full), BF16)],
        ),
        compiler_params=params,
        name="attention_forward",
    )(off, block_input, wa, vec, qvb, bias, pm, pmt)

    rows = imgs * trow
    out, gx1, gwb, ghb, sums_b = pl.pallas_call(
        functools.partial(feed_kernel, imgs=imgs, groups=groups, gc=gc, trow=trow, tokens=tokens),
        out_shape=(
            jax.ShapeDtypeStruct((mine, tokens, d), BF16),
            jax.ShapeDtypeStruct((mine * trow, d), F32),
            jax.ShapeDtypeStruct(wb.shape, BF16),
            jax.ShapeDtypeStruct((groups, 1, hid), F32),
            jax.ShapeDtypeStruct((8, d), F32),
        ),
        grid_spec=pltpu.PrefetchScalarGridSpec(
            num_scalar_prefetch=1,
            grid=(steps,),
            in_specs=[
                img_spec, img_spec, rows_spec(rows, full), whole(wb.shape), whole(vec.shape),
                whole(hb.shape),
            ],
            out_specs=[
                out_img_spec, rows_spec(rows, d), whole(wb.shape), whole(hb.shape), whole((8, d)),
            ],
            scratch_shapes=[
                pltpu.VMEM((rows, d), F32), pltpu.VMEM((rows, d), F32), pltpu.VMEM((rows, d), BF16),
                pltpu.VMEM((d, rows), BF16), pltpu.VMEM((d, rows), BF16),
                pltpu.VMEM((rows, d), F32), pltpu.VMEM((rows, d), F32),
                pltpu.VMEM((d, full), F32), pltpu.VMEM((groups, d, hid), F32),
                pltpu.VMEM((groups, d, hid), F32),
            ],
        ),
        compiler_params=params,
        name="feed_forward",
    )(off, block_input, out_grad, attn, wb, vec, hb)

    wp_spec = pl.BlockSpec((groups, d, gc), lambda i, o: (0, 0, 0), pipeline_mode=pl.Buffered(1))
    gin, gwa, gtab, gqv, sums_c = pl.pallas_call(
        functools.partial(
            attention_back_kernel, imgs=imgs, groups=groups, gh=gh, prow=prow, trow=trow, tokens=tokens
        ),
        out_shape=(
            jax.ShapeDtypeStruct((mine, tokens, d), BF16),
            jax.ShapeDtypeStruct((groups, d, 3 * gc), BF16),
            jax.ShapeDtypeStruct((groups, WPAD, gh * WPAD), F32),
            jax.ShapeDtypeStruct((8, full), F32),
            jax.ShapeDtypeStruct((8, d), F32),
        ),
        grid_spec=pltpu.PrefetchScalarGridSpec(
            num_scalar_prefetch=1,
            grid=(steps,),
            in_specs=[
                img_spec, rows_spec(rows, d), rows_spec(imgs * prow, 3 * full),
                rows_spec(imgs * prow, d), probs_spec, whole(wa.shape), wp_spec, whole(vec.shape),
                whole(pmp.shape), whole(pmt.shape),
            ],
            out_specs=[
                out_img_spec, whole((groups, d, 3 * gc)), whole((groups, WPAD, gh * WPAD)),
                whole((8, full)), whole((8, d)),
            ],
            scratch_shapes=[
                pltpu.VMEM((imgs * prow, d), BF16), pltpu.VMEM((imgs * prow, full), BF16),
                pltpu.VMEM((imgs * prow, 3 * full), BF16), pltpu.VMEM((d, imgs * prow), BF16),
                pltpu.VMEM((3, d, full), F32),
            ],
        ),
        compiler_params=params,
        name="attention_backward",
    )(off, block_input, gx1, qkv, hw, probs, wa, wb, vec, pmp, pmt)

    block_output = lax.all_gather(out, "mp", axis=0, tiled=True)
    input_grad = lax.all_gather(gin, "mp", axis=0, tiled=True)

    def scatter(g):
        part = lax.psum_scatter(g, "dp", scatter_dimension=1, tiled=True)
        return lax.psum_scatter(part, "mp", scatter_dimension=0, tiled=True)[0].astype(F32)

    gb = scatter(gwb)
    ga = scatter(gwa)
    gtab = gtab.reshape(groups, WPAD, gh, WPAD).transpose(0, 2, 1, 3).reshape(heads, WPAD * WPAD)
    gtab = lax.dot_general(gtab, one_hot, (((1,), (1,)), ((), ())), precision=lax.Precision.HIGHEST)
    sizes = [gtab.size, 2 * full, groups * hid, 2 * d, 4 * d]
    smalls = jnp.concatenate(
        [
            gtab.reshape(-1), gqv[0:2].reshape(-1), ghb.reshape(-1),
            sums_c[0], sums_b[0], sums_c[1], sums_b[1], sums_b[2], sums_b[3],
        ]
    )
    smalls = lax.psum(smalls, ("dp", "mp"))
    ends = np.cumsum(sizes)
    me = lax.axis_index("mp")
    my_rows = lax.axis_index("dp") * rows_w
    table_grad = lax.dynamic_slice_in_dim(smalls[0 : ends[0]].reshape(heads, table_len), me * gh, gh, 0)
    qv_grad = lax.dynamic_slice_in_dim(smalls[ends[0] : ends[1]].reshape(2, full), me * gc, gc, 1)
    hb_grad = lax.dynamic_slice_in_dim(smalls[ends[1] : ends[2]], me * hid, hid, 0)
    gains_grad = lax.dynamic_slice_in_dim(smalls[ends[2] : ends[3]].reshape(2, d), my_rows, rows_w, 1).T
    offs_grad = lax.dynamic_slice_in_dim(smalls[ends[3] : ends[4]].reshape(4, d), my_rows, rows_w, 1).T
    return (
        block_output, input_grad, gains_grad, offs_grad, ga.reshape(rows_w, 3, gc), qv_grad,
        table_grad, gb[:, 0:gc], gb[:, gc : gc + hid], hb_grad, gb[:, gc + hid : gc + 2 * hid],
    )


def solution(mesh):
    in_specs = (
        P("dp", None, None), P("dp", None, None), P("dp", None), P("dp", None), P("dp", None, "mp"),
        P(None, "mp"), P("mp", None), P("dp", "mp"), P("dp", "mp"), P("mp"), P("dp", "mp"), P(), P(),
    )
    out_specs = (
        P("dp", None, None), P("dp", None, None), P("dp", None), P("dp", None), P("dp", None, "mp"),
        P(None, "mp"), P("mp", None), P("dp", "mp"), P("dp", "mp"), P("mp"), P("dp", "mp"),
    )
    body = functools.partial(shards, n_dp=mesh.shape["dp"], n_mp=mesh.shape["mp"])
    return jax.shard_map(body, mesh=mesh, in_specs=in_specs, out_specs=out_specs, check_vma=False)
```

```python
import functools
import math

import jax
import jax.numpy as jnp
import numpy as np
from jax import lax
from jax.experimental import pallas as pl
from jax.experimental.pallas import tpu as pltpu
from jax.sharding import PartitionSpec as P

HD = 32
WIN = 7
SHIFT = 3
SIDE = 14
F32 = jnp.float32
BF16 = jnp.bfloat16
WPAD = 64
EPS = 1e-05
DEAD = -1e30


def dot(a, b, ca=1, cb=0):
    return lax.dot_general(a, b, (((ca,), (cb,)), ((), ())), preferred_element_type=F32)


def padded_order(shift):
    sides = SIDE // WIN
    wpos = WIN * WIN
    rows = np.full((sides * sides * WPAD,), -1, np.int32)
    for wr in range(sides):
        for wc in range(sides):
            for a in range(wpos):
                r = (wr * WIN + a // WIN + shift) % SIDE
                c = (wc * WIN + a % WIN + shift) % SIDE
                rows[(wr * sides + wc) * WPAD + a] = r * SIDE + c
    return rows


def pick_matrix(tokens, shift=SHIFT):
    rows = padded_order(shift)
    return (rows[:, None] == np.arange(tokens)[None, :]).astype(np.float32)


def norm(x):
    mean = jnp.mean(x, axis=-1, keepdims=True)
    cen = x - mean
    var = jnp.mean(cen * cen, axis=-1, keepdims=True)
    inv = lax.rsqrt(var + EPS)
    return cen * inv, inv


def norm_back(grad, normed, inv, gain):
    scaled = grad * gain
    return inv * (
        scaled
        - jnp.mean(scaled, axis=-1, keepdims=True)
        - normed * jnp.mean(scaled * normed, axis=-1, keepdims=True)
    )


def col_sum(v):
    return jnp.sum(v, axis=0, keepdims=True)


def head_masks(group_heads):
    lane_q = lax.broadcasted_iota(jnp.int32, (group_heads * WPAD, group_heads * HD), 0)
    lane_c = lax.broadcasted_iota(jnp.int32, (group_heads * WPAD, group_heads * HD), 1)
    return (lane_q // WPAD) == (lane_c // HD)


def spread(rows, mask, group_heads):
    tiled = jnp.concatenate([rows] * group_heads, axis=0)
    return jnp.where(mask, tiled, jnp.zeros_like(tiled))


def gather_heads(full, mask, group_heads):
    kept = jnp.where(mask, full, 0.0)
    total = kept[0:WPAD]
    for h in range(1, group_heads):
        total = total + kept[h * WPAD : (h + 1) * WPAD]
    return total


def vectors(vec_ref):
    return vec_ref[0].astype(F32).T


def attention_kernel(
    x_ref, w_ref, vec_ref, sm_ref, pos_ref, pen_ref, pm_ref, pmt_ref,
    *rest, imgs, groups, gh, prow, trow,
):
    qkv_ref, hw_ref, probs_ref, attn_ref, attw = rest[-5:]
    gc = gh * HD
    full = groups * gc
    vec = vectors(vec_ref)
    gain = vec[0:1, :]
    shift = vec[2:3, :]
    q_bias = jnp.concatenate([sm_ref[g, 0:1, :] for g in range(groups)], axis=1)
    v_bias = jnp.concatenate([sm_ref[g, 1:2, :] for g in range(groups)], axis=1)
    for im in range(imgs):
        normed, _ = norm(x_ref[im].astype(F32))
        h1 = (normed * gain + shift).astype(BF16)
        hw_ref[im * prow : (im + 1) * prow, :] = dot(pm_ref[...], h1).astype(BF16)
    hw = hw_ref[...]
    for kind in range(3):
        wk = jnp.concatenate([w_ref[g, :, kind * gc : (kind + 1) * gc] for g in range(groups)], axis=1)
        part = dot(hw, wk)
        if kind == 0:
            part = (part + q_bias) * (HD**-0.5)
        if kind == 2:
            part = part + v_bias
        qkv_ref[:, kind * full : (kind + 1) * full] = part.astype(BF16)
    wins = prow // WPAD
    mask = head_masks(gh)

    def window(i, carry):
        rows = pl.ds(pl.multiple_of(i * WPAD, WPAD), WPAD)
        win = lax.rem(i, wins)
        for g in range(groups):
            q = qkv_ref[rows, g * gc : (g + 1) * gc]
            k = qkv_ref[rows, full + g * gc : full + (g + 1) * gc]
            v = qkv_ref[rows, 2 * full + g * gc : 2 * full + (g + 1) * gc]
            scores = dot(k, spread(q, mask, gh), 1, 1) + (pos_ref[g] + pen_ref[win])
            e = jnp.exp(scores - jnp.max(scores, axis=0, keepdims=True))
            p = e * (1.0 / jnp.sum(e, axis=0, keepdims=True))
            probs_ref[i, g] = p
            o = gather_heads(dot(p.astype(BF16), v, 0, 0), mask, gh)
            attw[rows, g * gc : (g + 1) * gc] = o.astype(BF16)
        return carry

    lax.fori_loop(0, imgs * wins, window, 0)
    for im in range(imgs):
        attn_ref[im * trow : (im + 1) * trow, :] = dot(
            pmt_ref[...], attw[im * prow : (im + 1) * prow, :]
        ).astype(BF16)


def gelu_parts(pre):
    cdf = 0.5 * (1.0 + lax.erf(pre * (1.0 / math.sqrt(2.0))))
    density = jnp.exp(-0.5 * pre * pre) * (1.0 / math.sqrt(2.0 * math.pi))
    return pre * cdf, cdf + pre * density


def feed_kernel(
    x_ref, gy_ref, attn_ref, w_ref, vec_ref, sm_ref,
    *rest, imgs, groups, gc, hid, trow, tokens,
):
    out_ref, gx1_ref, act_ref, gpb_ref, h2_ref, gyp_ref, gb_ref, sums_ref, xs, gys, mlp, gh2 = rest[-12:]
    vec = vectors(vec_ref)

    @pl.when(pl.program_id(0) == 0)
    def _():
        gb_ref[...] = jnp.zeros_like(gb_ref)
        sums_ref[...] = jnp.zeros_like(sums_ref)

    xs[...] = jnp.zeros_like(xs)
    gys[...] = jnp.zeros_like(gys)
    for im in range(imgs):
        xs[im * trow : im * trow + tokens, :] = x_ref[im].astype(F32)
        gys[im * trow : im * trow + tokens, :] = gy_ref[im].astype(F32)
    proj = jnp.concatenate([w_ref[g, :, 0:gc] for g in range(groups)], axis=1)
    x1 = xs[...] + dot(attn_ref[...], proj, 1, 1) + vec[3:4, :]
    xs[...] = x1
    normed2, inv2 = norm(x1)
    h2_ref[...] = (normed2 * vec[1:2, :] + vec[4:5, :]).astype(BF16)
    gyp_ref[...] = gys[...].astype(BF16)
    mlp[...] = jnp.zeros_like(mlp)
    gh2[...] = jnp.zeros_like(gh2)

    for g in range(groups):
        fc1 = w_ref[g, :, gc : gc + hid]
        fc2 = w_ref[g, :, gc + hid : gc + 2 * hid]
        pre = dot(h2_ref[...], fc1) + jnp.concatenate(
            [sm_ref[g, 2 + k : 3 + k, :] for k in range(hid // 128)], axis=1
        )
        act, slope = gelu_parts(pre)
        act = act.astype(BF16)
        act_ref[:, g * hid : (g + 1) * hid] = act
        gpre = dot(gyp_ref[...], fc2) * slope
        gpb = gpre.astype(BF16)
        gpb_ref[:, g * hid : (g + 1) * hid] = gpb
        gb_ref[g] += col_sum(gpre)
        mlp[...] += dot(act, fc2, 1, 1)
        gh2[...] += dot(gpb, fc1, 1, 1)

    out = xs[...] + mlp[...] + vec[5:6, :]
    for im in range(imgs):
        out_ref[im] = out[im * trow : im * trow + tokens].astype(BF16)
    normed2, inv2 = norm(xs[...])
    grad = gh2[...]
    gy = gys[...]
    gx1 = gy + norm_back(grad, normed2, inv2, vec[1:2, :])
    gx1_ref[...] = gx1
    sums_ref[0:1, :] += col_sum(grad * normed2)
    sums_ref[1:2, :] += col_sum(gx1)
    sums_ref[2:3, :] += col_sum(grad)
    sums_ref[3:4, :] += col_sum(gy)


def attention_back_kernel(
    x_ref, gx1_ref, qkv_ref, probs_ref, wa_ref, wp_ref, vec_ref, pm_ref, pmt_ref,
    gin_ref, gqkv, table_ref, qvs_ref, sums_ref,
    gxw, ga, *, imgs, groups, gh, prow, trow, tokens, middle,
):
    step = pl.program_id(0)
    gc = gh * HD
    full = groups * gc

    gain = vectors(vec_ref)[0:1, :]

    @pl.when(step == 0)
    def _():
        table_ref[...] = jnp.zeros_like(table_ref)
        qvs_ref[...] = jnp.zeros_like(qvs_ref)
        sums_ref[...] = jnp.zeros_like(sums_ref)

    for im in range(imgs):
        gxw[im * prow : (im + 1) * prow, :] = dot(
            pm_ref[...], gx1_ref[im * trow : (im + 1) * trow, :].astype(BF16)
        ).astype(BF16)
    proj = jnp.concatenate([wp_ref[g, :, 0:gc] for g in range(groups)], axis=1)
    ga[...] = dot(gxw[...], proj).astype(BF16)
    mask = head_masks(gh)
    wins = prow // WPAD

    def window(i, carry):
        rows = pl.ds(pl.multiple_of(i * WPAD, WPAD), WPAD)
        all_rows = pl.ds(pl.multiple_of(step * imgs * prow + i * WPAD, WPAD), WPAD)
        for g in range(groups):
            cols = slice(g * gc, (g + 1) * gc)
            q = qkv_ref[rows, g * gc : (g + 1) * gc]
            k = qkv_ref[rows, full + g * gc : full + (g + 1) * gc]
            v = qkv_ref[rows, 2 * full + g * gc : 2 * full + (g + 1) * gc]
            p = probs_ref[i, g]
            gas = spread(ga[rows, cols], mask, gh)
            dp = dot(v, gas, 1, 1)
            ds = p * (dp - jnp.sum(p * dp, axis=0, keepdims=True))
            table_ref[g] += ds
            dsb = ds.astype(BF16)
            gq = gather_heads(dot(dsb, k, 0, 0), mask, gh) * (HD**-0.5)
            gk = dot(dsb, spread(q, mask, gh))
            gv = dot(p.astype(BF16), gas)
            qvs_ref[0:1, cols] += col_sum(gq)
            qvs_ref[1:2, cols] += col_sum(gv)
            gqkv[0, all_rows, cols] = gq.astype(BF16)
            gqkv[1, all_rows, cols] = gk.astype(BF16)
            gqkv[2, all_rows, cols] = gv.astype(BF16)
        return carry

    lax.fori_loop(0, imgs * wins, window, 0)
    middle()
    now = pl.ds(pl.multiple_of(step * imgs * prow, prow), imgs * prow)
    gh1 = None
    for kind in range(3):
        wk = jnp.concatenate([wa_ref[g, :, kind * gc : (kind + 1) * gc] for g in range(groups)], axis=1)
        term = dot(gqkv[kind, now, :], wk, 1, 1)
        gh1 = term if gh1 is None else gh1 + term
    gh1b = gh1.astype(BF16)
    for im in range(imgs):
        grad = dot(pmt_ref[...], gh1b[im * prow : (im + 1) * prow])[0:tokens]
        normed, inv = norm(x_ref[im].astype(F32))
        sums_ref[0:1, :] += col_sum(grad * normed)
        sums_ref[1:2, :] += col_sum(grad)
        gx0 = gx1_ref[im * trow : im * trow + tokens, :] + norm_back(grad, normed, inv, gain)
        gin_ref[im] = gx0.astype(BF16)


class Relay:
    def __init__(self, src, dst, sems, n_mp, passed):
        self.src, self.dst, self.n, self.passed = src, dst, n_mp, passed
        self.own_sem, self.send_sem, self.recv_sem, self.far_sem = sems
        self.m, self.me = lax.axis_index("mp"), lax.axis_index("dp")
        self.pieces = src.shape[0]

    @staticmethod
    def scratch(pieces, n_mp):
        dma = pltpu.SemaphoreType.DMA
        return [dma, dma((n_mp, pieces, 2)), dma((n_mp, pieces)), dma((n_mp, pieces))]

    def copy(self, s, p, step, own):
        return pltpu.make_async_remote_copy(
            src_ref=self.src.at[p] if own else self.dst.at[s, p], dst_ref=self.dst.at[s, p],
            send_sem=self.send_sem.at[s, p, (step + 1) // 2], recv_sem=self.recv_sem.at[s, p],
            device_id=(self.me, self.m + step), device_id_type=pl.DeviceIdType.MESH,
        )

    def far(self, p, j):
        to = lax.rem(self.m + j, self.n)
        return pltpu.make_async_remote_copy(
            src_ref=self.src.at[p], dst_ref=self.dst.at[self.m, p], send_sem=self.far_sem.at[j, p],
            recv_sem=self.recv_sem.at[self.m, p], device_id=(self.me, to),
            device_id_type=pl.DeviceIdType.MESH,
        )

    def edge(self, step):
        return self.m < self.n - 1 if step == 1 else self.m > 0

    def own_copy(self):
        return pltpu.make_async_copy(self.src, self.dst.at[self.m], self.own_sem)

    def start(self, greet=True):
        if greet:
            barrier = pltpu.get_barrier_semaphore()
            for j in range(1, self.n):
                pl.semaphore_signal(
                    barrier, inc=1, device_id=(self.me, lax.rem(self.m + j, self.n)),
                    device_id_type=pl.DeviceIdType.MESH,
                )
            pl.semaphore_wait(barrier, self.n - 1)
        for p in range(self.passed):
            for step in (1, -1):
                pl.when(self.edge(step))(lambda p=p, step=step: self.copy(self.m, p, step, True).start())
        for p in range(self.passed, self.pieces):
            for j in range(1, self.n):
                self.far(p, j).start()
        self.own_copy().start()

    def arrivals(self, k):
        return ((self.m - k, 1, self.m - k >= 0), (self.m + k, -1, self.m + k < self.n))

    def pass_one(self, k, p):
        for s, step, there in self.arrivals(k):

            def go(s=s, step=step):
                self.copy(s, p, step, False).wait_recv()
                pl.when(self.edge(step))(lambda: self.copy(s, p, step, False).start())

            pl.when(there)(go)

    def pass_on(self, k):
        for p in range(self.passed):
            self.pass_one(k, p)

    def finish(self):
        self.own_copy().wait()
        for p in range(self.passed, self.pieces):
            for j in range(1, self.n):
                self.far(p, j).wait_send()
                self.copy(lax.rem(self.m + j, self.n), p, 1, False).wait_recv()
        for p in range(self.passed):
            for step in (1, -1):
                pl.when(self.edge(step))(lambda p=p, step=step: self.copy(self.m, p, step, True).wait_send())
            for k in range(1, self.n):
                for s, step, there in self.arrivals(k):
                    pl.when(there & self.edge(step))(
                        lambda s=s, step=step, p=p: self.copy(s, p, step, False).wait_send()
                    )


def forward_kernel(*refs, imgs, groups, gh, gc, hid, prow, trow, tokens, kept, n_mp, relayed):
    refs = list(refs)
    x, gy, wa, wb, vec, sm, pos, pen, pm, pmt = refs[:10]
    refs = refs[10 + kept :]
    source = refs.pop(0) if relayed else None
    qkv, hw, probs, attn, out, gx1, act, gpb, h2, gyp, gb, sums = refs[:12]
    refs = refs[12:]
    target = refs.pop(0) if relayed else None
    attw, xs, gys, mlp, gh2 = refs[:5]
    step = pl.program_id(0)
    last = pl.num_programs(0) - 1
    relay = Relay(source, target, refs[5:], n_mp, 0) if relayed else None

    if relayed:
        pl.when(step == 0)(relay.start)
    attention_kernel(
        x, wa, vec, sm, pos, pen, pm, pmt, qkv, hw, probs, attn, attw,
        imgs=imgs, groups=groups, gh=gh, prow=prow, trow=trow,
    )
    feed_kernel(
        x, gy, attn, wb, vec, sm, out, gx1, act, gpb, h2, gyp, gb, sums, xs, gys, mlp, gh2,
        imgs=imgs, groups=groups, gc=gc, hid=hid, trow=trow, tokens=tokens,
    )
    if relayed:
        pl.when(step == last)(relay.finish)


def backward_kernel(*refs, imgs, steps, groups, gh, gc, hid, prow, trow, tokens, n_mp):
    refs = list(refs)
    x, gx1, qkv, probs, wa, wp, vec, pmp, pmt = refs[:9]
    hw, gx1_all, attn, h2, gpb, gyp, act, sums_1, sums_2, source = refs[9:19]
    gin, table, qvs, gw, target = refs[19:24]
    gqkv, sums, gxw, ga, vsum, hwt, gxt, h2t, gyt = refs[24:33]
    relay = Relay(source, target, refs[33:], n_mp, source.shape[0])
    todo = [(k, p) for k in range(1, n_mp) for p in range(relay.pieces)]

    def hook(at):
        return lambda: relay.pass_one(*todo[at])

    placed = max(0, min(2 * steps - 1, len(todo) - relay.pieces))

    def middle():
        for j in range(1, steps):
            if 2 * j - 1 < placed:
                pl.when(step == j)(hook(2 * j - 1))

    step = pl.program_id(0)

    @pl.when(step == 0)
    def _():
        relay.start()

    @pl.when(step < steps)
    def _():
        attention_back_kernel(
            x, gx1, qkv, probs, wa, wp, vec, pmp, pmt, gin, gqkv, table, qvs, sums, gxw, ga,
            imgs=imgs, groups=groups, gh=gh, prow=prow, trow=trow, tokens=tokens, middle=middle,
        )

    for j in range(steps):
        if 2 * j < placed:
            pl.when(step == j)(hook(2 * j))

    @pl.when(step >= steps)
    def _():
        g = step - steps

        @pl.when(g == 0)
        def _():
            hwt[...] = hw[...].astype(F32).T.astype(BF16)
            gxt[...] = gx1_all[...].T.astype(BF16)
            h2t[...] = h2[...].astype(F32).T.astype(BF16)
            gyt[...] = gyp[...].astype(F32).T.astype(BF16)
            vsum[...] = jnp.zeros_like(vsum)
            vsum[0:1, :] = sums[0:1, :]
            vsum[1:2, :] = sums_1[0:1, :] + sums_2[0:1, :]
            vsum[2:3, :] = sums[1:2, :]
            vsum[3:6, :] = sums_1[1:4, :] + sums_2[1:4, :]

        cols = pl.ds(pl.multiple_of(g * gc, gc), gc)
        for kind in range(3):
            gw[0, :, kind * gc : (kind + 1) * gc] = dot(hwt[...], gqkv[kind, :, cols]).astype(BF16)
        at = 3 * gc
        gw[0, :, at : at + gc] = dot(gxt[...], attn[...]).astype(BF16)
        at += gc
        gw[0, :, at : at + hid] = dot(h2t[...], gpb[...]).astype(BF16)
        at += hid
        gw[0, :, at : at + hid] = dot(gyt[...], act[...]).astype(BF16)
        at += hid
        gw[0, :, at : at + vsum.shape[0]] = vsum[...].T.astype(BF16)

    @pl.when(step == steps + groups - 1)
    def _():
        for k, p in todo[placed:]:
            relay.pass_one(k, p)
        relay.finish()


def coords(n_dp):
    nb = n_dp.bit_length() - 1
    me = lax.axis_index("dp")
    return nb, me, [(me // (1 << (nb - 1 - p))) % 2 for p in range(nb)]


def flipped(me, cs, nb, p):
    return me + (1 - 2 * cs[p]) * (1 << (nb - 1 - p))


def at_dp(idx):
    return {"dp": idx}


def meet(n_dp, n_mp):
    nb, me, cs = coords(n_dp)
    m = lax.axis_index("mp")
    barrier = pltpu.get_barrier_semaphore()
    for p in range(nb):
        pl.semaphore_signal(
            barrier, inc=1, device_id=(flipped(me, cs, nb, p), m), device_id_type=pl.DeviceIdType.MESH
        )
    for j in range(1, n_mp):
        pl.semaphore_signal(
            barrier, inc=1, device_id=(me, lax.rem(m + j, n_mp)), device_id_type=pl.DeviceIdType.MESH
        )
    pl.semaphore_wait(barrier, nb + n_mp - 1)


def halves_order(nb):
    first = list(range(nb))
    second = list(range(nb))
    if nb > 1:
        second[0], second[1] = 1, 0
    return [first, second]


def gather_kernel(
    in_ref, sm_ref, rel_ref, tab_ref, reg_ref, sel_ref, selt_ref,
    out_ref, smo_ref, pos_ref, pen_ref,
    own_pos, own_sem, z_send, z_recv, st_send, st_recv, x_send, x_recv, *, n_dp, n_mp, wpos,
):
    nb, me, cs = coords(n_dp)
    m = lax.axis_index("mp")
    rows = in_ref.shape[0]
    orders = halves_order(nb)
    cut = [pl.ds(0, rows // 2), pl.ds(rows // 2, rows // 2)]
    meet(n_dp, n_mp)

    def slot(s, free=(), flip=None):
        idx = [slice(None) if p in free else (1 - cs[p] if p == flip else cs[p]) for p in range(nb)]
        return (s, *idx)

    own = pltpu.make_async_copy(in_ref, out_ref.at[slot(m)], own_sem)
    own.start()

    def z_copy(s, step, src):
        return pltpu.make_async_remote_copy(
            src_ref=src, dst_ref=out_ref.at[slot(s)], send_sem=z_send.at[s, (step + 1) // 2],
            recv_sem=z_recv.at[s], device_id=(me, m + step), device_id_type=pl.DeviceIdType.MESH,
        )

    def stage(s, half, t, mine=False, arriving=False):
        p = orders[half][t]
        region = slot(s, tuple(orders[half][:t]), p if arriving else None) + (cut[half],)
        src = in_ref.at[cut[half]] if mine else out_ref.at[region]
        return pltpu.make_async_remote_copy(
            src_ref=src, dst_ref=out_ref.at[region], send_sem=st_send.at[s, half, t],
            recv_sem=st_recv.at[s, half, t], device_id=(flipped(me, cs, nb, p), m),
            device_id_type=pl.DeviceIdType.MESH,
        )

    def guarded(ok, fn):
        if ok is None:
            fn()
        else:
            pl.when(ok)(fn)

    items = [[(m, 0, None)]]
    for k in range(1, n_mp):
        items.append([(m - k, 1, m - k >= 0), (m + k, -1, m + k < n_mp)])

    def forward(s, way, wait):
        for step in (1, -1) if way == 0 else (way,):
            edge = m < n_mp - 1 if step == 1 else m > 0

            def go(step=step):
                c = z_copy(s, step, in_ref if way == 0 else out_ref.at[slot(s)])
                c.wait_send() if wait else c.start()

            pl.when(edge)(go)

    def advance(s, way, t):
        if t == 0:
            if way != 0:
                z_copy(s, way, out_ref.at[slot(s)]).wait_recv()
            forward(s, way, False)
        for half in range(2):
            if t > 0:
                stage(s, half, t - 1, arriving=True).wait_recv()
            if t < nb:
                stage(s, half, t, mine=(t == 0 and way == 0)).start()

    def expand(t, total):
        return jnp.where(rel_ref[...] == t, tab_ref[pl.ds(t, 1), :], total)

    def x_copies(j):
        to = lax.rem(m + j, n_mp)
        pairs = ((sm_ref, smo_ref), (own_pos, pos_ref))
        return [
            pltpu.make_async_remote_copy(
                src_ref=src, dst_ref=dst.at[m], send_sem=x_send.at[k, j - 1],
                recv_sem=x_recv.at[k, j - 1], device_id=(me, to), device_id_type=pl.DeviceIdType.MESH,
            )
            for k, (src, dst) in enumerate(pairs)
        ]

    def x_arrivals(j):
        frm = lax.rem(m + n_mp - j, n_mp)
        pairs = ((sm_ref, smo_ref), (own_pos, pos_ref))
        return [
            pltpu.make_async_remote_copy(
                src_ref=src, dst_ref=dst.at[frm], send_sem=x_send.at[k, j - 1],
                recv_sem=x_recv.at[k, j - 1], device_id=(me, frm), device_id_type=pl.DeviceIdType.MESH,
            )
            for k, (src, dst) in enumerate(pairs)
        ]

    def small_work():
        own_pos[...] = lax.fori_loop(
            0, tab_ref.shape[0], expand, jnp.zeros(own_pos.shape, F32)
        )
        for j in range(1, n_mp):
            for c in x_copies(j):
                c.start()
        smo_ref[m] = sm_ref[...]
        pos_ref[m] = own_pos[...]
        by_key = dot(sel_ref[...], reg_ref[...], 1, 1)
        by_query = dot(reg_ref[...], selt_ref[...])
        cols = own_pos.shape[1]
        key = lax.broadcasted_iota(jnp.int32, own_pos.shape, 0)
        for w in range(pen_ref.shape[0]):
            same = by_key[w * WPAD : (w + 1) * WPAD, 0:1] == by_query[0:1, w * cols : (w + 1) * cols]
            pen_ref[w] = jnp.where(key < wpos, jnp.where(same, 0.0, -100.0), DEAD)

    for tick in range(n_mp + nb - 1):
        if tick == 1:
            small_work()
            own.wait()
        for t in reversed(range(nb)):
            k = tick - t
            if 0 <= k < n_mp:
                for s, way, ok in items[k]:
                    guarded(ok, functools.partial(advance, s, way, t))
    for group in items:
        for s, way, ok in group:
            guarded(ok, functools.partial(advance, s, way, nb))
    for j in range(1, n_mp):
        for c in x_arrivals(j):
            c.wait_recv()
        for c in x_copies(j):
            c.wait_send()
    for group in items:
        for s, way, ok in group:

            def finish(s=s, way=way):
                forward(s, way, True)
                for half in range(2):
                    for t in range(nb):
                        stage(s, half, t, mine=(t == 0 and way == 0)).wait_send()

            guarded(ok, finish)


def reduce_kernel(
    g_ref, rel_ref, tab_ref, qvs_ref, gb1_ref, gb2_ref, gin_ref, o_ref, so_ref, all_ref,
    t_rows, sm_ref, *rest, n_dp, n_mp, table_len, gh, gc,
):
    nb, me, cs = coords(n_dp)
    relay = Relay(gin_ref, all_ref, rest[-4:], n_mp, gin_ref.shape[0])
    rest = rest[:-4]
    m = lax.axis_index("mp")
    rows = g_ref.shape[-2]
    half_rows = rows // 2
    rest = list(rest)
    recv = [[rest.pop(0) for _ in range(nb)] for _ in range(2)]
    acc = [[rest.pop(0) for _ in range(nb)] for _ in range(2)]
    zin = [rest.pop(0) for _ in range(2)]
    s_in, s_acc, s_zin = rest.pop(0), rest.pop(0), rest.pop(0)
    send_sem, recv_sem, z_send, z_recv, s_send, s_recv, sz_send, sz_recv = rest
    orders = [list(reversed(o)) for o in halves_order(nb)]
    meet(n_dp, n_mp)

    def remote(src, dst, ssem, rsem, device):
        return pltpu.make_async_remote_copy(
            src_ref=src, dst_ref=dst, send_sem=ssem, recv_sem=rsem, device_id=device,
            device_id_type=pl.DeviceIdType.MESH,
        )

    def region(half, t, mine):
        left = sorted(set(range(nb)) - set(orders[half][:t]))
        p = orders[half][t]
        idx = [slice(None)] + [(cs[p] if mine else 1 - cs[p]) if q == p else slice(None) for q in left]
        if t == 0:
            idx.append(pl.ds(half * half_rows, half_rows))
        return tuple(idx)

    def source(half, t):
        return g_ref if t == 0 else acc[half][t - 1]

    def copy(half, t):
        p = orders[half][t]
        return remote(
            source(half, t).at[region(half, t, False)], recv[half][t], send_sem.at[half, t],
            recv_sem.at[half, t], (flipped(me, cs, nb, p), m),
        )

    def s_copy(t):
        src = sm_ref if t == 0 else s_acc.at[t - 1]
        return remote(src, s_in.at[t], s_send.at[t], s_recv.at[t], (flipped(me, cs, nb, t), m))

    def z_copy(half, j):
        to = lax.rem(m + j, n_mp)
        return remote(
            acc[half][nb - 1].at[to], zin[half].at[j - 1], z_send.at[half, j - 1],
            z_recv.at[half, j - 1], (me, to),
        )

    def sz_copy(j):
        to = lax.rem(m + j, n_mp)
        return remote(
            s_acc.at[nb - 1, to], s_zin.at[j - 1], sz_send.at[j - 1], sz_recv.at[j - 1], (me, to)
        )

    relay.start(greet=False)
    for half in range(2):
        copy(half, 0).start()

    t_rows[...] = jnp.zeros_like(t_rows)

    def pick(t, carry):
        hit = rel_ref[...] == t
        for g in range(n_mp):
            t_rows[g, pl.ds(t, 1), :] = col_sum(jnp.where(hit, tab_ref[g], 0.0))
        return carry

    lax.fori_loop(0, table_len, pick, 0)
    lane = lax.broadcasted_iota(jnp.int32, (t_rows.shape[1], 128), 1)
    width = gh * WPAD
    for g in range(n_mp):
        total = jnp.zeros(lane.shape, F32)
        for h in range(gh):
            part = jnp.sum(t_rows[g, :, h * WPAD : (h + 1) * WPAD], axis=1, keepdims=True)
            total = jnp.where(lane == h, part, total)
        sm_ref[g] = jnp.zeros_like(sm_ref[g])
        sm_ref[g, 0:8, :] = total.T[0:8, 0:width]
        cols = slice(g * gc, (g + 1) * gc)
        sm_ref[g, 8:9, :] = jnp.concatenate([qvs_ref[0:1, cols], qvs_ref[1:2, cols]], axis=1)
        hidden = gb1_ref[g] + gb2_ref[g]
        for k in range(hidden.shape[1] // width):
            sm_ref[g, 9 + k : 10 + k, :] = hidden[:, k * width : (k + 1) * width]
    s_copy(0).start()
    for t in range(nb):
        for half in range(2):
            copy(half, t).wait_recv()
            src = source(half, t)
            keep = region(half, t, True)
            deep = nb - 1 - t

            def add(s, carry, half=half, t=t, src=src, keep=keep, deep=deep):
                for k in range(1 << deep):
                    bits = [(k >> (deep - 1 - q)) & 1 for q in range(deep)]
                    inner = list(bits)
                    idx = [s] + [inner.pop(0) if isinstance(v, slice) else v for v in keep[1 : 1 + deep + 1]]
                    if t == 0:
                        idx.append(keep[-1])
                    mine = src[tuple(idx)].astype(F32)
                    other = recv[half][t][(s, *bits)].astype(F32)
                    acc[half][t][(s, *bits)] = (mine + other).astype(BF16)
                return carry

            lax.fori_loop(0, n_mp, add, 0)
            if t + 1 < nb:
                copy(half, t + 1).start()
            else:
                for j in range(1, n_mp):
                    z_copy(half, j).start()
        s_copy(t).wait_recv()
        before = sm_ref[...] if t == 0 else s_acc[t - 1]
        s_acc[t] = before + s_in[t]
        if t + 1 < nb:
            s_copy(t + 1).start()
        else:
            for j in range(1, n_mp):
                sz_copy(j).start()
        if t < n_mp - 1:
            relay.pass_on(t + 1)
    for k in range(nb + 1, n_mp):
        relay.pass_on(k)
    for half in range(2):
        total = acc[half][nb - 1][m].astype(F32)
        for j in range(1, n_mp):
            z_copy(half, j).wait_recv()
            total = total + zin[half][j - 1].astype(F32)
        o_ref[half * half_rows : (half + 1) * half_rows, :] = total
    s_total = s_acc[nb - 1, m]
    for j in range(1, n_mp):
        sz_copy(j).wait_recv()
        s_total = s_total + s_zin[j - 1]
    so_ref[...] = s_total
    for half in range(2):
        for t in range(nb):
            copy(half, t).wait_send()
        for j in range(1, n_mp):
            z_copy(half, j).wait_send()
    for t in range(nb):
        s_copy(t).wait_send()
    for j in range(1, n_mp):
        sz_copy(j).wait_send()
    relay.finish()


def unpack_kernel(
    red_ref, small_ref, gains_ref, offs_ref, qkv_ref, qv_ref, table_ref, proj_ref, fc1_ref, hb_ref, fc2_ref,
):
    gc = proj_ref.shape[1]
    hid = fc1_ref.shape[1]
    for kind in range(3):
        qkv_ref[kind] = red_ref[:, kind * gc : (kind + 1) * gc]
    at = 3 * gc
    proj_ref[...] = red_ref[:, at : at + gc]
    at += gc
    fc1_ref[...] = red_ref[:, at : at + hid]
    at += hid
    fc2_ref[...] = red_ref[:, at : at + hid]
    at += hid
    vec = red_ref[:, at : at + 128].T
    gains_ref[...] = vec[0:2]
    offs_ref[...] = vec[2:6]
    table_ref[...] = small_ref[0 : table_ref.shape[0], 0 : table_ref.shape[1]]
    qv_ref[0:1, :] = small_ref[8:9, 0:gc]
    qv_ref[1:2, :] = small_ref[8:9, gc : 2 * gc]
    for k in range(hid // (2 * gc)):
        hb_ref[:, k * 2 * gc : (k + 1) * 2 * gc] = small_ref[9 + k : 10 + k, :]


def gather_all(pack, small, rel, tab, reg, sel, selt, wpos, wins, n_dp, n_mp):
    nb = n_dp.bit_length() - 1
    rows, cols = pack.shape
    dma = pltpu.SemaphoreType.DMA
    shaped = jax.ShapeDtypeStruct
    vmem = pl.BlockSpec(memory_space=pltpu.VMEM)
    got, smalls, pos, pen = pl.pallas_call(
        functools.partial(gather_kernel, n_dp=n_dp, n_mp=n_mp, wpos=wpos),
        out_shape=(
            shaped((n_mp,) + (2,) * nb + (rows, cols), pack.dtype), shaped((n_mp,) + small.shape, F32),
            shaped((n_mp,) + rel.shape, F32), shaped((wins,) + rel.shape, F32),
        ),
        in_specs=[vmem] * 7,
        out_specs=[pl.BlockSpec(memory_space=pl.ANY), vmem, vmem, vmem],
        scratch_shapes=[
            pltpu.VMEM(rel.shape, F32),
            dma, dma((n_mp, 2)), dma((n_mp,)), dma((n_mp, 2, nb)), dma((n_mp, 2, nb)),
            dma((2, n_mp - 1)), dma((2, n_mp - 1)),
        ],
        compiler_params=pltpu.CompilerParams(collective_id=0, has_side_effects=True),
        name="gather_weights",
    )(pack, small, rel, tab, reg, sel, selt)
    return got.reshape(n_mp, n_dp * rows, cols), smalls, pos, pen


def reduce_all(grads, rel, tab, qvs, gb1, gb2, gin, n_dp, n_mp, table_len, gh, gc):
    nb = n_dp.bit_length() - 1
    _, d, cols = grads.shape
    rows = d // n_dp
    half = rows // 2
    dma = pltpu.SemaphoreType.DMA
    parts = [pltpu.VMEM((n_mp,) + (2,) * (nb - 1 - t) + (half, cols), BF16) for t in range(nb)]
    sr, sc = 16, gh * WPAD
    assert sc == 2 * gc and 9 + gb1.shape[2] // sc <= sr and table_len <= sc
    return pl.pallas_call(
        functools.partial(
            reduce_kernel, n_dp=n_dp, n_mp=n_mp, table_len=table_len, gh=gh, gc=gc
        ),
        out_shape=(
            jax.ShapeDtypeStruct((rows, cols), F32), jax.ShapeDtypeStruct((sr, sc), F32),
            jax.ShapeDtypeStruct((n_mp,) + gin.shape, BF16),
        ),
        in_specs=[pl.BlockSpec(memory_space=pltpu.VMEM)] * 7,
        out_specs=[pl.BlockSpec(memory_space=pltpu.VMEM)] * 2 + [pl.BlockSpec(memory_space=pl.ANY)],
        scratch_shapes=[pltpu.VMEM((n_mp, sc, sc), F32), pltpu.VMEM((n_mp, sr, sc), F32)]
        + parts * 4
        + [pltpu.VMEM((n_mp - 1, half, cols), BF16)] * 2
        + [pltpu.VMEM((nb, n_mp, sr, sc), F32)] * 2
        + [pltpu.VMEM((n_mp - 1, sr, sc), F32)]
        + [dma((2, nb))] * 2 + [dma((2, n_mp - 1))] * 2 + [dma((nb,))] * 2 + [dma((n_mp - 1,))] * 2
        + Relay.scratch(gin.shape[0], n_mp),
        compiler_params=pltpu.CompilerParams(
            collective_id=1, has_side_effects=True, vmem_limit_bytes=60 * 1024 * 1024
        ),
        name="reduce_gradients",
    )(grads.reshape((n_mp,) + (2,) * nb + (rows, cols)), rel, tab, qvs, gb1, gb2, gin)


def whole(shape):
    zero = (0,) * len(shape)
    return pl.BlockSpec(shape, lambda i: zero, pipeline_mode=pl.Buffered(1))


def shards(
    block_input, out_grad, norm_gains, offsets, qkv_weight, qv_bias, pos_table,
    proj_weight, fc1_weight, fc1_bias, fc2_weight, rel_index, region_ids, *, n_dp, n_mp,
):
    images, tokens, d = block_input.shape
    groups = n_mp
    gh, table_len = pos_table.shape
    gc = gh * HD
    hid = fc1_bias.shape[0]
    heads = groups * gh
    rows_w = qkv_weight.shape[0]
    wpos = rel_index.shape[0]
    wins = tokens // wpos
    prow = wins * WPAD
    trow = -(-tokens // 16) * 16
    mine = images // n_mp
    imgs = 2 if mine % 2 == 0 else 1
    steps = mine // imgs
    m = lax.axis_index("mp")

    n_vec = norm_gains.shape[1] + offsets.shape[1]
    pack = jnp.concatenate(
        [
            proj_weight, fc1_weight, fc2_weight, qkv_weight.reshape(rows_w, 3 * gc), norm_gains,
            offsets, jnp.zeros((rows_w, 128 - n_vec), BF16),
        ],
        axis=1,
    )
    qkv_at = (gc + 2 * hid) // (3 * gc)
    vec_at = (4 * gc + 2 * hid) // 128
    assert qkv_at * 3 * gc == gc + 2 * hid and gc == 128
    small = jnp.concatenate([qv_bias.reshape(-1), fc1_bias]).astype(F32).reshape(-1, 128)
    small = jnp.pad(small, ((0, -small.shape[0] % 8), (0, 0)))
    pad_w = WPAD - wpos
    rel_t = jnp.pad(rel_index.T, ((0, pad_w), (0, pad_w)), constant_values=-1)
    rel = jnp.tile(rel_t, (1, gh))
    tab = jnp.repeat(pos_table.T, WPAD, axis=1)
    reg = jnp.broadcast_to(region_ids.reshape(1, -1), (8, tokens)).astype(BF16)
    plain = pick_matrix(tokens, 0)
    selt = np.tile(plain.T.reshape(tokens, wins, 1, WPAD), (1, 1, gh, 1)).reshape(tokens, -1)
    got, smalls_in, pos, pen = gather_all(
        pack, small, rel, tab, reg, jnp.asarray(plain, BF16), jnp.asarray(selt, BF16), wpos, wins,
        n_dp, n_mp,
    )

    pick = pick_matrix(tokens)
    pick_pad = np.pad(pick, ((0, 0), (0, trow - tokens)))
    pm = jnp.asarray(pick, BF16)
    pmp = jnp.asarray(pick_pad, BF16)
    pmt = jnp.asarray(pick_pad.T, BF16)
    full = groups * gc
    x_mine = lax.dynamic_slice_in_dim(block_input, m * mine, mine, 0)
    gy_mine = lax.dynamic_slice_in_dim(out_grad, m * mine, mine, 0)
    rows = imgs * trow
    prows = imgs * prow
    wa_spec = pl.BlockSpec((groups, d, 3 * gc), lambda i: (0, 0, qkv_at), pipeline_mode=pl.Buffered(1))
    wb_spec = pl.BlockSpec((groups, d, gc + 2 * hid), lambda i: (0, 0, 0), pipeline_mode=pl.Buffered(1))
    wp_spec = pl.BlockSpec((groups, d, gc), lambda i: (0, 0, 0), pipeline_mode=pl.Buffered(1))
    any_spec = pl.BlockSpec(memory_space=pl.ANY)

    def part_spec(shape, c):
        tail = (0,) * (len(shape) - 1)
        return pl.BlockSpec(shape, lambda i, c=c: (c + i, *tail))

    vec_spec = pl.BlockSpec((1, d, 128), lambda i: (0, 0, vec_at), pipeline_mode=pl.Buffered(1))
    shaped = jax.ShapeDtypeStruct
    names = dict(
        imgs=imgs, groups=groups, gh=gh, gc=gc, hid=hid, prow=prow, trow=trow, tokens=tokens, n_mp=n_mp
    )
    big = (
        shaped((mine * prow, 3 * full), BF16), shaped((mine * prow, d), BF16),
        shaped((mine * wins, groups, WPAD, gh * WPAD), F32), shaped((mine * trow, full), BF16),
    )
    big_fed = (
        shaped((mine * trow, d), F32), shaped((mine * trow, groups * hid), BF16),
        shaped((mine * trow, groups * hid), BF16), shaped((mine * trow, d), BF16),
        shaped((mine * trow, d), BF16),
    )
    probs_block = (imgs * wins, groups, WPAD, gh * WPAD)
    sent, kept, ghbs, sums_bs, arrived = [], [], [], [], []
    first = 0
    for count in (1, steps - 1):
        c = first
        first += count
        relayed = len(sent) > 0
        got_back = pl.pallas_call(
            functools.partial(forward_kernel, kept=len(kept), relayed=relayed, **names),
            out_shape=big + (shaped((count, imgs, tokens, d), BF16),) + big_fed
            + (shaped((groups, 1, hid), F32), shaped((8, d), F32))
            + ((shaped((n_mp,) + sent[0].shape, BF16),) if relayed else ()),
            grid=(count,),
            in_specs=[
                part_spec((imgs, tokens, d), c), part_spec((imgs, tokens, d), c), wa_spec, wb_spec,
                vec_spec, whole(smalls_in.shape), whole(pos.shape), whole(pen.shape), whole(pm.shape),
                whole(pmt.shape),
            ] + [any_spec] * len(kept) + ([whole(sent[0].shape)] if relayed else []),
            out_specs=[
                part_spec((prows, 3 * full), c), part_spec((prows, d), c), part_spec(probs_block, c),
                part_spec((rows, full), c),
                pl.BlockSpec((None, imgs, tokens, d), lambda i: (i, 0, 0, 0)),
                part_spec((rows, d), c), part_spec((rows, groups * hid), c),
                part_spec((rows, groups * hid), c), part_spec((rows, d), c), part_spec((rows, d), c),
                whole((groups, 1, hid)), whole((8, d)),
            ] + ([any_spec] if relayed else []),
            scratch_shapes=[pltpu.VMEM((prows, full), BF16)] + [pltpu.VMEM((rows, d), F32)] * 4
            + (Relay.scratch(sent[0].shape[0], n_mp) if relayed else []),
            input_output_aliases={10 + k: k if k < 4 else k + 1 for k in range(len(kept))},
            compiler_params=pltpu.CompilerParams(
                vmem_limit_bytes=60 * 1024 * 1024,
                **(dict(collective_id=2, has_side_effects=True) if relayed else {}),
            ),
            name="forward",
        )(x_mine, gy_mine, got, got, got, smalls_in, pos, pen, pm, pmt, *kept, *sent)
        kept = list(got_back[0:4]) + list(got_back[5:10])
        sent = [got_back[4]]
        ghbs.append(got_back[10])
        sums_bs.append(got_back[11])
        arrived += got_back[12:]
    qkv, hw, probs, attn, gx1, act, gpb, h2, gyp = kept
    gcols = 4 * gc + 2 * hid + 128

    def early(shape):
        tail = (0,) * (len(shape) - 1)
        return pl.BlockSpec(shape, lambda i: (jnp.minimum(i, steps - 1), *tail))

    def late(r, c):
        return pl.BlockSpec((r, c), lambda i: (0, jnp.maximum(i - steps, 0)))

    trows_all, prows_all = mine * trow, mine * prow
    gin, gtab, gqv, gw, out_2 = pl.pallas_call(
        functools.partial(backward_kernel, steps=steps, **names),
        out_shape=(
            shaped((mine, tokens, d), BF16), shaped((groups, WPAD, gh * WPAD), F32),
            shaped((8, full), F32), shaped((groups, d, gcols), BF16),
            shaped((n_mp,) + sent[0].shape, BF16),
        ),
        grid=(steps + groups,),
        in_specs=[
            early((imgs, tokens, d)), early((rows, d)), early((prows, 3 * full)), early(probs_block),
            wa_spec, wp_spec, vec_spec, whole(pmp.shape), whole(pmt.shape), whole(hw.shape),
            whole(gx1.shape), late(trows_all, gc), whole(h2.shape), late(trows_all, hid),
            whole(gyp.shape), late(trows_all, hid), whole((8, d)), whole((8, d)), any_spec,
        ],
        out_specs=[
            early((imgs, tokens, d)), whole((groups, WPAD, gh * WPAD)), whole((8, full)),
            pl.BlockSpec((1, d, gcols), lambda i: (jnp.maximum(i - steps, 0), 0, 0)), any_spec,
        ],
        scratch_shapes=[
            pltpu.VMEM((3, prows_all, full), BF16), pltpu.VMEM((8, d), F32),
            pltpu.VMEM((prows, d), BF16), pltpu.VMEM((prows, full), BF16), pltpu.VMEM((128, d), F32),
            pltpu.VMEM((d, prows_all), BF16), pltpu.VMEM((d, trows_all), BF16),
            pltpu.VMEM((d, trows_all), BF16), pltpu.VMEM((d, trows_all), BF16),
        ] + Relay.scratch(sent[0].shape[0], n_mp),
        compiler_params=pltpu.CompilerParams(
            vmem_limit_bytes=60 * 1024 * 1024, collective_id=3, has_side_effects=True
        ),
        name="backward",
    )(
        x_mine, gx1, qkv, probs, got, got, got, pmp, pmt, hw, gx1, attn, h2, gpb, gyp, act, *sums_bs,
        *sent,
    )
    arrived.append(out_2)
    red, red_s, input_grad = reduce_all(
        gw, rel, gtab, gqv, *ghbs, gin.reshape(steps, imgs, tokens, d), n_dp, n_mp, table_len, gh, gc
    )
    input_grad = input_grad.reshape(images, tokens, d)
    out_parts = arrived
    block_output = jnp.concatenate(out_parts, axis=1).reshape(images, tokens, d)
    gains_t, offs_t, qkv_t, qv_grad, table_grad, proj_grad, fc1_grad, hb_grad, fc2_grad = pl.pallas_call(
        unpack_kernel,
        out_shape=tuple(
            shaped(shape, F32)
            for shape in (
                (2, rows_w), (4, rows_w), (3, rows_w, gc), (2, gc), (gh, table_len), (rows_w, gc),
                (rows_w, hid), (1, hid), (rows_w, hid),
            )
        ),
        name="unpack",
    )(red, red_s)
    return (
        block_output, input_grad, gains_t.T, offs_t.T, qkv_t.transpose(1, 0, 2), qv_grad, table_grad,
        proj_grad, fc1_grad, hb_grad.reshape(hid), fc2_grad,
    )


def solution(mesh):
    in_specs = (
        P("dp", None, None), P("dp", None, None), P("dp", None), P("dp", None), P("dp", None, "mp"),
        P(None, "mp"), P("mp", None), P("dp", "mp"), P("dp", "mp"), P("mp"), P("dp", "mp"), P(), P(),
    )
    out_specs = (
        P("dp", None, None), P("dp", None, None), P("dp", None), P("dp", None), P("dp", None, "mp"),
        P(None, "mp"), P("mp", None), P("dp", "mp"), P("dp", "mp"), P("mp"), P("dp", "mp"),
    )
    body = functools.partial(shards, n_dp=mesh.shape["dp"], n_mp=mesh.shape["mp"])
    return jax.shard_map(body, mesh=mesh, in_specs=in_specs, out_specs=out_specs, check_vma=False)
```

```python
import functools
import math

import jax
import jax.numpy as jnp
import numpy as np
from jax import lax
from jax.experimental import pallas as pl
from jax.experimental.pallas import tpu as pltpu
from jax.sharding import PartitionSpec as P

HD = 32
WIN = 7
SHIFT = 3
SIDE = 14
F32 = jnp.float32
BF16 = jnp.bfloat16
WPAD = 64
EPS = 1e-05
DEAD = -1e30


def dot(a, b, ca=1, cb=0):
    return lax.dot_general(a, b, (((ca,), (cb,)), ((), ())), preferred_element_type=F32)


def padded_order(shift):
    sides = SIDE // WIN
    wpos = WIN * WIN
    rows = np.full((sides * sides * WPAD,), -1, np.int32)
    for wr in range(sides):
        for wc in range(sides):
            for a in range(wpos):
                r = (wr * WIN + a // WIN + shift) % SIDE
                c = (wc * WIN + a % WIN + shift) % SIDE
                rows[(wr * sides + wc) * WPAD + a] = r * SIDE + c
    return rows


def pick_matrix(tokens, shift=SHIFT):
    rows = padded_order(shift)
    return (rows[:, None] == np.arange(tokens)[None, :]).astype(np.float32)


def norm(x):
    mean = jnp.mean(x, axis=-1, keepdims=True)
    cen = x - mean
    var = jnp.mean(cen * cen, axis=-1, keepdims=True)
    inv = lax.rsqrt(var + EPS)
    return cen * inv, inv


def norm_back(grad, normed, inv, gain):
    scaled = grad * gain
    return inv * (
        scaled
        - jnp.mean(scaled, axis=-1, keepdims=True)
        - normed * jnp.mean(scaled * normed, axis=-1, keepdims=True)
    )


def col_sum(v):
    return jnp.sum(v, axis=0, keepdims=True)


def head_masks(group_heads):
    lane_q = lax.broadcasted_iota(jnp.int32, (group_heads * WPAD, group_heads * HD), 0)
    lane_c = lax.broadcasted_iota(jnp.int32, (group_heads * WPAD, group_heads * HD), 1)
    return (lane_q // WPAD) == (lane_c // HD)


def spread(rows, mask, group_heads):
    tiled = jnp.concatenate([rows] * group_heads, axis=0)
    return jnp.where(mask, tiled, jnp.zeros_like(tiled))


def gather_heads(full, mask, group_heads):
    kept = jnp.where(mask, full, 0.0)
    total = kept[0:WPAD]
    for h in range(1, group_heads):
        total = total + kept[h * WPAD : (h + 1) * WPAD]
    return total


def vectors(vec_ref):
    return vec_ref[0].astype(F32).T


def attention_kernel(
    x_ref, w_ref, vec_ref, sm_ref, pos_ref, pen_ref, pm_ref, pmt_ref,
    *rest, imgs, groups, gh, prow, trow,
):
    qkv_ref, hw_ref, probs_ref, attn_ref, attw = rest[-5:]
    gc = gh * HD
    full = groups * gc
    vec = vectors(vec_ref)
    gain = vec[0:1, :]
    shift = vec[2:3, :]
    q_bias = jnp.concatenate([sm_ref[g, 0:1, :] for g in range(groups)], axis=1)
    v_bias = jnp.concatenate([sm_ref[g, 1:2, :] for g in range(groups)], axis=1)
    for im in range(imgs):
        normed, _ = norm(x_ref[im].astype(F32))
        h1 = (normed * gain + shift).astype(BF16)
        hw_ref[im * prow : (im + 1) * prow, :] = dot(pm_ref[...], h1).astype(BF16)
    hw = hw_ref[...]
    for kind in range(3):
        wk = jnp.concatenate([w_ref[g, :, kind * gc : (kind + 1) * gc] for g in range(groups)], axis=1)
        part = dot(hw, wk)
        if kind == 0:
            part = (part + q_bias) * (HD**-0.5)
        if kind == 2:
            part = part + v_bias
        qkv_ref[:, kind * full : (kind + 1) * full] = part.astype(BF16)
    wins = prow // WPAD
    mask = head_masks(gh)

    def window(i, carry):
        rows = pl.ds(pl.multiple_of(i * WPAD, WPAD), WPAD)
        win = lax.rem(i, wins)
        for g in range(groups):
            q = qkv_ref[rows, g * gc : (g + 1) * gc]
            k = qkv_ref[rows, full + g * gc : full + (g + 1) * gc]
            v = qkv_ref[rows, 2 * full + g * gc : 2 * full + (g + 1) * gc]
            scores = dot(k, spread(q, mask, gh), 1, 1) + (pos_ref[g] + pen_ref[win])
            e = jnp.exp(scores - jnp.max(scores, axis=0, keepdims=True))
            p = e * (1.0 / jnp.sum(e, axis=0, keepdims=True))
            probs_ref[i, g] = p
            o = gather_heads(dot(p.astype(BF16), v, 0, 0), mask, gh)
            attw[rows, g * gc : (g + 1) * gc] = o.astype(BF16)
        return carry

    lax.fori_loop(0, imgs * wins, window, 0)
    for im in range(imgs):
        attn_ref[im * trow : (im + 1) * trow, :] = dot(
            pmt_ref[...], attw[im * prow : (im + 1) * prow, :]
        ).astype(BF16)


def gelu_parts(pre):
    cdf = 0.5 * (1.0 + lax.erf(pre * (1.0 / math.sqrt(2.0))))
    density = jnp.exp(-0.5 * pre * pre) * (1.0 / math.sqrt(2.0 * math.pi))
    return pre * cdf, cdf + pre * density


def feed_kernel(
    x_ref, gy_ref, attn_ref, w_ref, vec_ref, sm_ref,
    *rest, imgs, groups, gc, hid, trow, tokens, middle,
):
    out_ref, gx1_ref, act_ref, gpb_ref, h2_ref, gyp_ref, gb_ref, sums_ref, xs, gys, mlp, gh2 = rest[-12:]
    vec = vectors(vec_ref)

    @pl.when(pl.program_id(0) == 0)
    def _():
        gb_ref[...] = jnp.zeros_like(gb_ref)
        sums_ref[...] = jnp.zeros_like(sums_ref)

    xs[...] = jnp.zeros_like(xs)
    gys[...] = jnp.zeros_like(gys)
    for im in range(imgs):
        xs[im * trow : im * trow + tokens, :] = x_ref[im].astype(F32)
        gys[im * trow : im * trow + tokens, :] = gy_ref[im].astype(F32)
    proj = jnp.concatenate([w_ref[g, :, 0:gc] for g in range(groups)], axis=1)
    x1 = xs[...] + dot(attn_ref[...], proj, 1, 1) + vec[3:4, :]
    xs[...] = x1
    normed2, inv2 = norm(x1)
    h2_ref[...] = (normed2 * vec[1:2, :] + vec[4:5, :]).astype(BF16)
    gyp_ref[...] = gys[...].astype(BF16)
    mlp[...] = jnp.zeros_like(mlp)
    gh2[...] = jnp.zeros_like(gh2)

    for g in range(groups):
        if g == groups // 2:
            middle()
        fc1 = w_ref[g, :, gc : gc + hid]
        fc2 = w_ref[g, :, gc + hid : gc + 2 * hid]
        pre = dot(h2_ref[...], fc1) + jnp.concatenate(
            [sm_ref[g, 2 + k : 3 + k, :] for k in range(hid // 128)], axis=1
        )
        act, slope = gelu_parts(pre)
        act = act.astype(BF16)
        act_ref[:, g * hid : (g + 1) * hid] = act
        gpre = dot(gyp_ref[...], fc2) * slope
        gpb = gpre.astype(BF16)
        gpb_ref[:, g * hid : (g + 1) * hid] = gpb
        gb_ref[g] += col_sum(gpre)
        mlp[...] += dot(act, fc2, 1, 1)
        gh2[...] += dot(gpb, fc1, 1, 1)

    out = xs[...] + mlp[...] + vec[5:6, :]
    for im in range(imgs):
        out_ref[im] = out[im * trow : im * trow + tokens].astype(BF16)
    normed2, inv2 = norm(xs[...])
    grad = gh2[...]
    gy = gys[...]
    gx1 = gy + norm_back(grad, normed2, inv2, vec[1:2, :])
    gx1_ref[...] = gx1
    sums_ref[0:1, :] += col_sum(grad * normed2)
    sums_ref[1:2, :] += col_sum(gx1)
    sums_ref[2:3, :] += col_sum(grad)
    sums_ref[3:4, :] += col_sum(gy)


def attention_back_kernel(
    x_ref, gx1_ref, qkv_ref, probs_ref, wa_ref, wp_ref, vec_ref, pm_ref, pmt_ref,
    gin_ref, gqkv, table_ref, qvs_ref, sums_ref,
    gxw, ga, *, imgs, groups, gh, prow, trow, tokens, middle,
):
    step = pl.program_id(0)
    gc = gh * HD
    full = groups * gc

    gain = vectors(vec_ref)[0:1, :]

    @pl.when(step == 0)
    def _():
        table_ref[...] = jnp.zeros_like(table_ref)
        qvs_ref[...] = jnp.zeros_like(qvs_ref)
        sums_ref[...] = jnp.zeros_like(sums_ref)

    for im in range(imgs):
        gxw[im * prow : (im + 1) * prow, :] = dot(
            pm_ref[...], gx1_ref[im * trow : (im + 1) * trow, :].astype(BF16)
        ).astype(BF16)
    proj = jnp.concatenate([wp_ref[g, :, 0:gc] for g in range(groups)], axis=1)
    ga[...] = dot(gxw[...], proj).astype(BF16)
    mask = head_masks(gh)
    wins = prow // WPAD

    def window(i, carry):
        rows = pl.ds(pl.multiple_of(i * WPAD, WPAD), WPAD)
        all_rows = pl.ds(pl.multiple_of(step * imgs * prow + i * WPAD, WPAD), WPAD)
        for g in range(groups):
            cols = slice(g * gc, (g + 1) * gc)
            q = qkv_ref[rows, g * gc : (g + 1) * gc]
            k = qkv_ref[rows, full + g * gc : full + (g + 1) * gc]
            v = qkv_ref[rows, 2 * full + g * gc : 2 * full + (g + 1) * gc]
            p = probs_ref[i, g]
            gas = spread(ga[rows, cols], mask, gh)
            dp = dot(v, gas, 1, 1)
            ds = p * (dp - jnp.sum(p * dp, axis=0, keepdims=True))
            table_ref[g] += ds
            dsb = ds.astype(BF16)
            gq = gather_heads(dot(dsb, k, 0, 0), mask, gh) * (HD**-0.5)
            gk = dot(dsb, spread(q, mask, gh))
            gv = dot(p.astype(BF16), gas)
            qvs_ref[0:1, cols] += col_sum(gq)
            qvs_ref[1:2, cols] += col_sum(gv)
            gqkv[0, all_rows, cols] = gq.astype(BF16)
            gqkv[1, all_rows, cols] = gk.astype(BF16)
            gqkv[2, all_rows, cols] = gv.astype(BF16)
        return carry

    lax.fori_loop(0, imgs * wins, window, 0)
    middle()
    now = pl.ds(pl.multiple_of(step * imgs * prow, prow), imgs * prow)
    gh1 = None
    for kind in range(3):
        wk = jnp.concatenate([wa_ref[g, :, kind * gc : (kind + 1) * gc] for g in range(groups)], axis=1)
        term = dot(gqkv[kind, now, :], wk, 1, 1)
        gh1 = term if gh1 is None else gh1 + term
    gh1b = gh1.astype(BF16)
    for im in range(imgs):
        grad = dot(pmt_ref[...], gh1b[im * prow : (im + 1) * prow])[0:tokens]
        normed, inv = norm(x_ref[im].astype(F32))
        sums_ref[0:1, :] += col_sum(grad * normed)
        sums_ref[1:2, :] += col_sum(grad)
        gx0 = gx1_ref[im * trow : im * trow + tokens, :] + norm_back(grad, normed, inv, gain)
        gin_ref[im] = gx0.astype(BF16)


class Relay:
    def __init__(self, src, dst, sems, n_mp, passed):
        self.src, self.dst, self.n, self.passed = src, dst, n_mp, passed
        self.own_sem, self.send_sem, self.recv_sem, self.far_sem = sems
        self.m, self.me = lax.axis_index("mp"), lax.axis_index("dp")
        self.pieces = src.shape[0]

    @staticmethod
    def scratch(pieces, n_mp):
        dma = pltpu.SemaphoreType.DMA
        return [dma, dma((n_mp, pieces, 2)), dma((n_mp, pieces)), dma((n_mp, pieces))]

    def copy(self, s, p, step, own):
        return pltpu.make_async_remote_copy(
            src_ref=self.src.at[p] if own else self.dst.at[s, p], dst_ref=self.dst.at[s, p],
            send_sem=self.send_sem.at[s, p, (step + 1) // 2], recv_sem=self.recv_sem.at[s, p],
            device_id=(self.me, self.m + step), device_id_type=pl.DeviceIdType.MESH,
        )

    def far(self, p, j):
        to = lax.rem(self.m + j, self.n)
        return pltpu.make_async_remote_copy(
            src_ref=self.src.at[p], dst_ref=self.dst.at[self.m, p], send_sem=self.far_sem.at[j, p],
            recv_sem=self.recv_sem.at[self.m, p], device_id=(self.me, to),
            device_id_type=pl.DeviceIdType.MESH,
        )

    def edge(self, step):
        return self.m < self.n - 1 if step == 1 else self.m > 0

    def own_copy(self):
        return pltpu.make_async_copy(self.src, self.dst.at[self.m], self.own_sem)

    def start(self, greet=True):
        if greet:
            barrier = pltpu.get_barrier_semaphore()
            for j in range(1, self.n):
                pl.semaphore_signal(
                    barrier, inc=1, device_id=(self.me, lax.rem(self.m + j, self.n)),
                    device_id_type=pl.DeviceIdType.MESH,
                )
            pl.semaphore_wait(barrier, self.n - 1)
        for p in range(self.passed):
            for step in (1, -1):
                pl.when(self.edge(step))(lambda p=p, step=step: self.copy(self.m, p, step, True).start())
        for p in range(self.passed, self.pieces):
            for j in range(1, self.n):
                self.far(p, j).start()
        self.own_copy().start()

    def arrivals(self, k):
        return ((self.m - k, 1, self.m - k >= 0), (self.m + k, -1, self.m + k < self.n))

    def pass_one(self, k, p):
        for s, step, there in self.arrivals(k):

            def go(s=s, step=step):
                self.copy(s, p, step, False).wait_recv()
                pl.when(self.edge(step))(lambda: self.copy(s, p, step, False).start())

            pl.when(there)(go)

    def pass_on(self, k):
        for p in range(self.passed):
            self.pass_one(k, p)

    def finish(self):
        self.own_copy().wait()
        for p in range(self.passed, self.pieces):
            for j in range(1, self.n):
                self.far(p, j).wait_send()
                self.copy(lax.rem(self.m + j, self.n), p, 1, False).wait_recv()
        for p in range(self.passed):
            for step in (1, -1):
                pl.when(self.edge(step))(lambda p=p, step=step: self.copy(self.m, p, step, True).wait_send())
            for k in range(1, self.n):
                for s, step, there in self.arrivals(k):
                    pl.when(there & self.edge(step))(
                        lambda s=s, step=step, p=p: self.copy(s, p, step, False).wait_send()
                    )


def forward_kernel(*refs, imgs, groups, gh, gc, hid, prow, trow, tokens, kept, n_mp, relayed):
    refs = list(refs)
    x, gy, wa, wb, vec, sm, pos, pen, pm, pmt = refs[:10]
    refs = refs[10 + kept :]
    source = refs.pop(0) if relayed else None
    qkv, hw, probs, attn, out, gx1, act, gpb, h2, gyp, gb, sums = refs[:12]
    refs = refs[12:]
    target = refs.pop(0) if relayed else None
    attw, xs, gys, mlp, gh2 = refs[:5]
    step = pl.program_id(0)
    last = pl.num_programs(0) - 1
    relay = Relay(source, target, refs[5:], n_mp, source.shape[0]) if relayed else None
    hooks = {(0, 1): (1, 0), (0, 2): (1, 1), (0, 3): (2, 0), (1, 1): (2, 1)}
    if relayed and (n_mp != 4 or relay.pieces != 2):
        hooks = {}
    done = [pair for pair in hooks.values()]

    def place(at):
        for (j, here), pair in hooks.items():
            if relayed and here == at:
                pl.when(step == j)(lambda pair=pair: relay.pass_one(*pair))


    if relayed:
        pl.when(step == 0)(relay.start)
    attention_kernel(
        x, wa, vec, sm, pos, pen, pm, pmt, qkv, hw, probs, attn, attw,
        imgs=imgs, groups=groups, gh=gh, prow=prow, trow=trow,
    )
    place(1)
    feed_kernel(
        x, gy, attn, wb, vec, sm, out, gx1, act, gpb, h2, gyp, gb, sums, xs, gys, mlp, gh2,
        imgs=imgs, groups=groups, gc=gc, hid=hid, trow=trow, tokens=tokens, middle=lambda: place(2),
    )
    place(3)
    if relayed:

        def finish():
            for k in range(1, n_mp):
                for p in range(relay.pieces):
                    if (k, p) not in done:
                        relay.pass_one(k, p)
            relay.finish()

        pl.when(step == last)(finish)


def backward_kernel(*refs, imgs, steps, groups, gh, gc, hid, prow, trow, tokens, n_mp):
    refs = list(refs)
    x, gx1, qkv, probs, wa, wp, vec, pmp, pmt = refs[:9]
    hw, gx1_all, attn, h2, gpb, gyp, act, sums_1, sums_2, source = refs[9:19]
    gin, table, qvs, gw, target = refs[19:24]
    gqkv, sums, gxw, ga, vsum, hwt, gxt, h2t, gyt = refs[24:33]
    relay = Relay(source, target, refs[33:], n_mp, source.shape[0])
    todo = [(k, p) for k in range(1, n_mp) for p in range(relay.pieces)]

    def hook(at):
        return lambda: relay.pass_one(*todo[at])

    step = pl.program_id(0)
    in_steps = {1: 1, 2: 2}
    at_ends = {0: 0, 3: 3}
    placed = 4
    if steps < 3 or relay.pieces != 2 or n_mp != 4:
        in_steps, at_ends, placed = {}, {}, 0

    def middle():
        for j, at in in_steps.items():
            pl.when(step == j)(hook(at))

    @pl.when(step == 0)
    def _():
        relay.start()

    @pl.when(step < steps)
    def _():
        attention_back_kernel(
            x, gx1, qkv, probs, wa, wp, vec, pmp, pmt, gin, gqkv, table, qvs, sums, gxw, ga,
            imgs=imgs, groups=groups, gh=gh, prow=prow, trow=trow, tokens=tokens, middle=middle,
        )

    def end_hooks(steps_here):
        for j, at in at_ends.items():
            if j in steps_here:
                pl.when(step == j)(hook(at))

    end_hooks(range(steps))

    @pl.when(step >= steps)
    def _():
        g = step - steps

        @pl.when(g == 0)
        def _():
            hwt[...] = hw[...].astype(F32).T.astype(BF16)
            gxt[...] = gx1_all[...].T.astype(BF16)
            h2t[...] = h2[...].astype(F32).T.astype(BF16)
            gyt[...] = gyp[...].astype(F32).T.astype(BF16)
            vsum[...] = jnp.zeros_like(vsum)
            vsum[0:1, :] = sums[0:1, :]
            vsum[1:2, :] = sums_1[0:1, :] + sums_2[0:1, :]
            vsum[2:3, :] = sums[1:2, :]
            vsum[3:6, :] = sums_1[1:4, :] + sums_2[1:4, :]

        cols = pl.ds(pl.multiple_of(g * gc, gc), gc)
        for kind in range(3):
            gw[0, :, kind * gc : (kind + 1) * gc] = dot(hwt[...], gqkv[kind, :, cols]).astype(BF16)
        at = 3 * gc
        gw[0, :, at : at + gc] = dot(gxt[...], attn[...]).astype(BF16)
        at += gc
        gw[0, :, at : at + hid] = dot(h2t[...], gpb[...]).astype(BF16)
        at += hid
        gw[0, :, at : at + hid] = dot(gyt[...], act[...]).astype(BF16)
        at += hid
        gw[0, :, at : at + vsum.shape[0]] = vsum[...].T.astype(BF16)

    end_hooks(range(steps, steps + groups))

    @pl.when(step == steps + groups - 1)
    def _():
        for k, p in todo[placed:]:
            relay.pass_one(k, p)
        relay.finish()


def coords(n_dp):
    nb = n_dp.bit_length() - 1
    me = lax.axis_index("dp")
    return nb, me, [(me // (1 << (nb - 1 - p))) % 2 for p in range(nb)]


def flipped(me, cs, nb, p):
    return me + (1 - 2 * cs[p]) * (1 << (nb - 1 - p))


def at_dp(idx):
    return {"dp": idx}


def meet(n_dp, n_mp):
    nb, me, cs = coords(n_dp)
    m = lax.axis_index("mp")
    barrier = pltpu.get_barrier_semaphore()
    for p in range(nb):
        pl.semaphore_signal(
            barrier, inc=1, device_id=(flipped(me, cs, nb, p), m), device_id_type=pl.DeviceIdType.MESH
        )
    for j in range(1, n_mp):
        pl.semaphore_signal(
            barrier, inc=1, device_id=(me, lax.rem(m + j, n_mp)), device_id_type=pl.DeviceIdType.MESH
        )
    pl.semaphore_wait(barrier, nb + n_mp - 1)


def halves_order(nb):
    first = list(range(nb))
    second = list(range(nb))
    if nb > 1:
        second[0], second[1] = 1, 0
    return [first, second]


def gather_kernel(
    in_ref, sm_ref, rel_in, tab_in, reg_ref, row_ref, col_ref,
    out_ref, smo_ref, pos_ref, pen_ref, rel_ref,
    own_pos, rel_pad, tab_pad, tab_ref, own_sem, z_send, z_recv, st_send, st_recv, x_send, x_recv, *, n_dp, n_mp, wpos,
):
    nb, me, cs = coords(n_dp)
    m = lax.axis_index("mp")
    rows = in_ref.shape[0]
    orders = halves_order(nb)
    cut = [pl.ds(0, rows // 2), pl.ds(rows // 2, rows // 2)]
    meet(n_dp, n_mp)

    def slot(s, free=(), flip=None):
        idx = [slice(None) if p in free else (1 - cs[p] if p == flip else cs[p]) for p in range(nb)]
        return (s, *idx)

    own = pltpu.make_async_copy(in_ref, out_ref.at[slot(m)], own_sem)
    own.start()

    def z_copy(s, step, src):
        return pltpu.make_async_remote_copy(
            src_ref=src, dst_ref=out_ref.at[slot(s)], send_sem=z_send.at[s, (step + 1) // 2],
            recv_sem=z_recv.at[s], device_id=(me, m + step), device_id_type=pl.DeviceIdType.MESH,
        )

    def stage(s, half, t, mine=False, arriving=False):
        p = orders[half][t]
        region = slot(s, tuple(orders[half][:t]), p if arriving else None) + (cut[half],)
        src = in_ref.at[cut[half]] if mine else out_ref.at[region]
        return pltpu.make_async_remote_copy(
            src_ref=src, dst_ref=out_ref.at[region], send_sem=st_send.at[s, half, t],
            recv_sem=st_recv.at[s, half, t], device_id=(flipped(me, cs, nb, p), m),
            device_id_type=pl.DeviceIdType.MESH,
        )

    def guarded(ok, fn):
        if ok is None:
            fn()
        else:
            pl.when(ok)(fn)

    items = [[(m, 0, None)]]
    for k in range(1, n_mp):
        items.append([(m - k, 1, m - k >= 0), (m + k, -1, m + k < n_mp)])

    def forward(s, way, wait):
        for step in (1, -1) if way == 0 else (way,):
            edge = m < n_mp - 1 if step == 1 else m > 0

            def go(step=step):
                c = z_copy(s, step, in_ref if way == 0 else out_ref.at[slot(s)])
                c.wait_send() if wait else c.start()

            pl.when(edge)(go)

    def advance(s, way, t):
        if t == 0:
            if way != 0:
                z_copy(s, way, out_ref.at[slot(s)]).wait_recv()
            forward(s, way, False)
        for half in range(2):
            if t > 0:
                stage(s, half, t - 1, arriving=True).wait_recv()
            if t < nb:
                stage(s, half, t, mine=(t == 0 and way == 0)).start()

    def expand(t, total):
        return jnp.where(rel_ref[...] == t, tab_ref[pl.ds(t, 1), :], total)

    def x_copies(j):
        to = lax.rem(m + j, n_mp)
        pairs = ((sm_ref, smo_ref), (own_pos, pos_ref))
        return [
            pltpu.make_async_remote_copy(
                src_ref=src, dst_ref=dst.at[m], send_sem=x_send.at[k, j - 1],
                recv_sem=x_recv.at[k, j - 1], device_id=(me, to), device_id_type=pl.DeviceIdType.MESH,
            )
            for k, (src, dst) in enumerate(pairs)
        ]

    def x_arrivals(j):
        frm = lax.rem(m + n_mp - j, n_mp)
        pairs = ((sm_ref, smo_ref), (own_pos, pos_ref))
        return [
            pltpu.make_async_remote_copy(
                src_ref=src, dst_ref=dst.at[frm], send_sem=x_send.at[k, j - 1],
                recv_sem=x_recv.at[k, j - 1], device_id=(me, frm), device_id_type=pl.DeviceIdType.MESH,
            )
            for k, (src, dst) in enumerate(pairs)
        ]

    def small_work():
        gh = tab_in.shape[0]
        rel_pad[...] = jnp.full(rel_pad.shape, -1.0, F32)
        rel_pad[0:wpos, 0:wpos] = rel_in[...].astype(F32)
        rel_t = rel_pad[...].T[0:WPAD, 0:WPAD]
        rel_ref[...] = jnp.concatenate([rel_t] * gh, axis=1).astype(jnp.int32)
        tab_pad[...] = jnp.zeros_like(tab_pad)
        tab_pad[0:gh, 0 : tab_in.shape[1]] = tab_in[...]
        tab_t = tab_pad[...].T
        tab_ref[...] = jnp.concatenate(
            [jnp.broadcast_to(tab_t[:, h : h + 1], (tab_t.shape[0], WPAD)) for h in range(gh)], axis=1
        )
        own_pos[...] = lax.fori_loop(
            0, tab_in.shape[1], expand, jnp.zeros(own_pos.shape, F32)
        )
        for j in range(1, n_mp):
            for c in x_copies(j):
                c.start()
        smo_ref[m] = sm_ref[...]
        pos_ref[m] = own_pos[...]
        picked = dot(row_ref[...], reg_ref[...].astype(F32).astype(BF16))
        by_key = jnp.sum(picked * col_ref[...], axis=1, keepdims=True)
        by_query = jnp.broadcast_to(by_key, (by_key.shape[0], 128)).T
        key = lax.broadcasted_iota(jnp.int32, own_pos.shape, 0)
        for w in range(pen_ref.shape[0]):
            here = slice(w * WPAD, (w + 1) * WPAD)
            same = by_key[here] == jnp.concatenate([by_query[0:1, here]] * gh, axis=1)
            pen_ref[w] = jnp.where(key < wpos, jnp.where(same, 0.0, -100.0), DEAD)

    for tick in range(n_mp + nb - 1):
        if tick == 1:
            small_work()
            own.wait()
        for t in reversed(range(nb)):
            k = tick - t
            if 0 <= k < n_mp:
                for s, way, ok in items[k]:
                    guarded(ok, functools.partial(advance, s, way, t))
    for group in items:
        for s, way, ok in group:
            guarded(ok, functools.partial(advance, s, way, nb))
    for j in range(1, n_mp):
        for c in x_arrivals(j):
            c.wait_recv()
        for c in x_copies(j):
            c.wait_send()
    for group in items:
        for s, way, ok in group:

            def finish(s=s, way=way):
                forward(s, way, True)
                for half in range(2):
                    for t in range(nb):
                        stage(s, half, t, mine=(t == 0 and way == 0)).wait_send()

            guarded(ok, finish)


def reduce_kernel(
    g_ref, rel_ref, tab_ref, qvs_ref, gb1_ref, gb2_ref, gin_ref, o_ref, so_ref, all_ref,
    t_rows, sm_ref, *rest, n_dp, n_mp, table_len, gh, gc,
):
    nb, me, cs = coords(n_dp)
    relay = Relay(gin_ref, all_ref, rest[-4:], n_mp, gin_ref.shape[0])
    rest = rest[:-4]
    m = lax.axis_index("mp")
    rows = g_ref.shape[-2]
    half_rows = rows // 2
    rest = list(rest)
    recv = [[rest.pop(0) for _ in range(nb)] for _ in range(2)]
    acc = [[rest.pop(0) for _ in range(nb)] for _ in range(2)]
    zin = [rest.pop(0) for _ in range(2)]
    s_in, s_acc, s_zin = rest.pop(0), rest.pop(0), rest.pop(0)
    send_sem, recv_sem, z_send, z_recv, s_send, s_recv, sz_send, sz_recv = rest
    orders = [list(reversed(o)) for o in halves_order(nb)]
    meet(n_dp, n_mp)

    def remote(src, dst, ssem, rsem, device):
        return pltpu.make_async_remote_copy(
            src_ref=src, dst_ref=dst, send_sem=ssem, recv_sem=rsem, device_id=device,
            device_id_type=pl.DeviceIdType.MESH,
        )

    def region(half, t, mine):
        left = sorted(set(range(nb)) - set(orders[half][:t]))
        p = orders[half][t]
        idx = [slice(None)] + [(cs[p] if mine else 1 - cs[p]) if q == p else slice(None) for q in left]
        if t == 0:
            idx.append(pl.ds(half * half_rows, half_rows))
        return tuple(idx)

    def source(half, t):
        return g_ref if t == 0 else acc[half][t - 1]

    def copy(half, t):
        p = orders[half][t]
        return remote(
            source(half, t).at[region(half, t, False)], recv[half][t], send_sem.at[half, t],
            recv_sem.at[half, t], (flipped(me, cs, nb, p), m),
        )

    def s_copy(t):
        src = sm_ref if t == 0 else s_acc.at[t - 1]
        return remote(src, s_in.at[t], s_send.at[t], s_recv.at[t], (flipped(me, cs, nb, t), m))

    def z_copy(half, j):
        to = lax.rem(m + j, n_mp)
        return remote(
            acc[half][nb - 1].at[to], zin[half].at[j - 1], z_send.at[half, j - 1],
            z_recv.at[half, j - 1], (me, to),
        )

    def sz_copy(j):
        to = lax.rem(m + j, n_mp)
        return remote(
            s_acc.at[nb - 1, to], s_zin.at[j - 1], sz_send.at[j - 1], sz_recv.at[j - 1], (me, to)
        )

    relay.start(greet=False)
    for half in range(2):
        copy(half, 0).start()

    t_rows[...] = jnp.zeros_like(t_rows)

    def pick(t, carry):
        hit = rel_ref[...] == t
        for g in range(n_mp):
            t_rows[g, pl.ds(t, 1), :] = col_sum(jnp.where(hit, tab_ref[g], 0.0))
        return carry

    lax.fori_loop(0, table_len, pick, 0)
    lane = lax.broadcasted_iota(jnp.int32, (t_rows.shape[1], 128), 1)
    width = gh * WPAD
    for g in range(n_mp):
        total = jnp.zeros(lane.shape, F32)
        for h in range(gh):
            part = jnp.sum(t_rows[g, :, h * WPAD : (h + 1) * WPAD], axis=1, keepdims=True)
            total = jnp.where(lane == h, part, total)
        sm_ref[g] = jnp.zeros_like(sm_ref[g])
        sm_ref[g, 0:8, :] = total.T[0:8, 0:width]
        cols = slice(g * gc, (g + 1) * gc)
        sm_ref[g, 8:9, :] = jnp.concatenate([qvs_ref[0:1, cols], qvs_ref[1:2, cols]], axis=1)
        hidden = gb1_ref[g] + gb2_ref[g]
        for k in range(hidden.shape[1] // width):
            sm_ref[g, 9 + k : 10 + k, :] = hidden[:, k * width : (k + 1) * width]
    s_copy(0).start()
    for t in range(nb):
        for half in range(2):
            copy(half, t).wait_recv()
            src = source(half, t)
            keep = region(half, t, True)
            deep = nb - 1 - t

            def add(s, carry, half=half, t=t, src=src, keep=keep, deep=deep):
                for k in range(1 << deep):
                    bits = [(k >> (deep - 1 - q)) & 1 for q in range(deep)]
                    inner = list(bits)
                    idx = [s] + [inner.pop(0) if isinstance(v, slice) else v for v in keep[1 : 1 + deep + 1]]
                    if t == 0:
                        idx.append(keep[-1])
                    mine = src[tuple(idx)].astype(F32)
                    other = recv[half][t][(s, *bits)].astype(F32)
                    acc[half][t][(s, *bits)] = (mine + other).astype(BF16)
                return carry

            lax.fori_loop(0, n_mp, add, 0)
            if t + 1 < nb:
                copy(half, t + 1).start()
            else:
                for j in range(1, n_mp):
                    z_copy(half, j).start()
        s_copy(t).wait_recv()
        before = sm_ref[...] if t == 0 else s_acc[t - 1]
        s_acc[t] = before + s_in[t]
        if t + 1 < nb:
            s_copy(t + 1).start()
        else:
            for j in range(1, n_mp):
                sz_copy(j).start()
        if t < n_mp - 1:
            relay.pass_on(t + 1)
    for k in range(nb + 1, n_mp):
        relay.pass_on(k)
    for half in range(2):
        total = acc[half][nb - 1][m].astype(F32)
        for j in range(1, n_mp):
            z_copy(half, j).wait_recv()
            total = total + zin[half][j - 1].astype(F32)
        o_ref[half * half_rows : (half + 1) * half_rows, :] = total
    s_total = s_acc[nb - 1, m]
    for j in range(1, n_mp):
        sz_copy(j).wait_recv()
        s_total = s_total + s_zin[j - 1]
    so_ref[...] = s_total
    for half in range(2):
        for t in range(nb):
            copy(half, t).wait_send()
        for j in range(1, n_mp):
            z_copy(half, j).wait_send()
    for t in range(nb):
        s_copy(t).wait_send()
    for j in range(1, n_mp):
        sz_copy(j).wait_send()
    relay.finish()


def unpack_kernel(
    red_ref, small_ref, gains_ref, offs_ref, qkv_ref, qv_ref, table_ref, proj_ref, fc1_ref, hb_ref, fc2_ref,
):
    gc = proj_ref.shape[1]
    hid = fc1_ref.shape[1]
    for kind in range(3):
        qkv_ref[kind] = red_ref[:, kind * gc : (kind + 1) * gc]
    at = 3 * gc
    proj_ref[...] = red_ref[:, at : at + gc]
    at += gc
    fc1_ref[...] = red_ref[:, at : at + hid]
    at += hid
    fc2_ref[...] = red_ref[:, at : at + hid]
    at += hid
    vec = red_ref[:, at : at + 128].T
    gains_ref[...] = vec[0:2]
    offs_ref[...] = vec[2:6]
    table_ref[...] = small_ref[0 : table_ref.shape[0], 0 : table_ref.shape[1]]
    qv_ref[0:1, :] = small_ref[8:9, 0:gc]
    qv_ref[1:2, :] = small_ref[8:9, gc : 2 * gc]
    for k in range(hid // (2 * gc)):
        hb_ref[:, k * 2 * gc : (k + 1) * 2 * gc] = small_ref[9 + k : 10 + k, :]


def gather_all(pack, small, rel, tab, reg, row, col, wpos, wins, n_dp, n_mp):
    nb = n_dp.bit_length() - 1
    rows, cols = pack.shape
    dma = pltpu.SemaphoreType.DMA
    shaped = jax.ShapeDtypeStruct
    vmem = pl.BlockSpec(memory_space=pltpu.VMEM)
    wide = (WPAD, tab.shape[0] * WPAD)
    assert tab.shape[1] <= 256 and tab.shape[0] <= 128
    got, smalls, pos, pen, rel_t = pl.pallas_call(
        functools.partial(gather_kernel, n_dp=n_dp, n_mp=n_mp, wpos=wpos),
        out_shape=(
            shaped((n_mp,) + (2,) * nb + (rows, cols), pack.dtype), shaped((n_mp,) + small.shape, F32),
            shaped((n_mp,) + wide, F32), shaped((wins,) + wide, F32), shaped(wide, jnp.int32),
        ),
        in_specs=[vmem] * 7,
        out_specs=[pl.BlockSpec(memory_space=pl.ANY), vmem, vmem, vmem, vmem],
        scratch_shapes=[
            pltpu.VMEM(wide, F32), pltpu.VMEM((128, 128), F32), pltpu.VMEM((128, 256), F32),
            pltpu.VMEM((256, wide[1]), F32),
            dma, dma((n_mp, 2)), dma((n_mp,)), dma((n_mp, 2, nb)), dma((n_mp, 2, nb)),
            dma((2, n_mp - 1)), dma((2, n_mp - 1)),
        ],
        compiler_params=pltpu.CompilerParams(collective_id=0, has_side_effects=True),
        name="gather_weights",
    )(pack, small, rel, tab, reg, row, col)
    return got.reshape(n_mp, n_dp * rows, cols), smalls, pos, pen, rel_t


def reduce_all(grads, rel, tab, qvs, gb1, gb2, gin, n_dp, n_mp, table_len, gh, gc):
    nb = n_dp.bit_length() - 1
    _, d, cols = grads.shape
    rows = d // n_dp
    half = rows // 2
    dma = pltpu.SemaphoreType.DMA
    parts = [pltpu.VMEM((n_mp,) + (2,) * (nb - 1 - t) + (half, cols), BF16) for t in range(nb)]
    sr, sc = 16, gh * WPAD
    assert sc == 2 * gc and 9 + gb1.shape[2] // sc <= sr and table_len <= sc
    return pl.pallas_call(
        functools.partial(
            reduce_kernel, n_dp=n_dp, n_mp=n_mp, table_len=table_len, gh=gh, gc=gc
        ),
        out_shape=(
            jax.ShapeDtypeStruct((rows, cols), F32), jax.ShapeDtypeStruct((sr, sc), F32),
            jax.ShapeDtypeStruct((n_mp,) + gin.shape, BF16),
        ),
        in_specs=[pl.BlockSpec(memory_space=pltpu.VMEM)] * 7,
        out_specs=[pl.BlockSpec(memory_space=pltpu.VMEM)] * 2 + [pl.BlockSpec(memory_space=pl.ANY)],
        scratch_shapes=[pltpu.VMEM((n_mp, sc, sc), F32), pltpu.VMEM((n_mp, sr, sc), F32)]
        + parts * 4
        + [pltpu.VMEM((n_mp - 1, half, cols), BF16)] * 2
        + [pltpu.VMEM((nb, n_mp, sr, sc), F32)] * 2
        + [pltpu.VMEM((n_mp - 1, sr, sc), F32)]
        + [dma((2, nb))] * 2 + [dma((2, n_mp - 1))] * 2 + [dma((nb,))] * 2 + [dma((n_mp - 1,))] * 2
        + Relay.scratch(gin.shape[0], n_mp),
        compiler_params=pltpu.CompilerParams(
            collective_id=1, has_side_effects=True, vmem_limit_bytes=60 * 1024 * 1024
        ),
        name="reduce_gradients",
    )(grads.reshape((n_mp,) + (2,) * nb + (rows, cols)), rel, tab, qvs, gb1, gb2, gin)


def whole(shape):
    zero = (0,) * len(shape)
    return pl.BlockSpec(shape, lambda i: zero, pipeline_mode=pl.Buffered(1))


def shards(
    block_input, out_grad, norm_gains, offsets, qkv_weight, qv_bias, pos_table,
    proj_weight, fc1_weight, fc1_bias, fc2_weight, rel_index, region_ids, *, n_dp, n_mp,
):
    images, tokens, d = block_input.shape
    groups = n_mp
    gh, table_len = pos_table.shape
    gc = gh * HD
    hid = fc1_bias.shape[0]
    heads = groups * gh
    rows_w = qkv_weight.shape[0]
    wpos = rel_index.shape[0]
    wins = tokens // wpos
    prow = wins * WPAD
    trow = -(-tokens // 16) * 16
    mine = images // n_mp
    imgs = 2 if mine % 2 == 0 else 1
    steps = mine // imgs
    m = lax.axis_index("mp")

    n_vec = norm_gains.shape[1] + offsets.shape[1]
    pack = jnp.concatenate(
        [
            proj_weight, fc1_weight, fc2_weight, qkv_weight.reshape(rows_w, 3 * gc), norm_gains,
            offsets, jnp.zeros((rows_w, 128 - n_vec), BF16),
        ],
        axis=1,
    )
    qkv_at = (gc + 2 * hid) // (3 * gc)
    vec_at = (4 * gc + 2 * hid) // 128
    assert qkv_at * 3 * gc == gc + 2 * hid and gc == 128
    small = jnp.concatenate([qv_bias.reshape(-1), fc1_bias]).astype(F32).reshape(-1, 128)
    small = jnp.pad(small, ((0, -small.shape[0] % 8), (0, 0)))
    plain = padded_order(0)
    cells = np.arange(SIDE)[None, :]
    real = plain[:, None] >= 0
    row = (real & (plain[:, None] // SIDE == cells)).astype(np.float32)
    col = (real & (plain[:, None] % SIDE == cells)).astype(np.float32)
    got, smalls_in, pos, pen, rel = gather_all(
        pack, small, rel_index, pos_table, region_ids, jnp.asarray(row, BF16), jnp.asarray(col, F32),
        wpos, wins, n_dp, n_mp,
    )

    pick = pick_matrix(tokens)
    pick_pad = np.pad(pick, ((0, 0), (0, trow - tokens)))
    pm = jnp.asarray(pick, BF16)
    pmp = jnp.asarray(pick_pad, BF16)
    pmt = jnp.asarray(pick_pad.T, BF16)
    full = groups * gc
    x_mine = lax.dynamic_slice_in_dim(block_input, m * mine, mine, 0)
    gy_mine = lax.dynamic_slice_in_dim(out_grad, m * mine, mine, 0)
    rows = imgs * trow
    prows = imgs * prow
    wa_spec = pl.BlockSpec((groups, d, 3 * gc), lambda i: (0, 0, qkv_at), pipeline_mode=pl.Buffered(1))
    wb_spec = pl.BlockSpec((groups, d, gc + 2 * hid), lambda i: (0, 0, 0), pipeline_mode=pl.Buffered(1))
    wp_spec = pl.BlockSpec((groups, d, gc), lambda i: (0, 0, 0), pipeline_mode=pl.Buffered(1))
    any_spec = pl.BlockSpec(memory_space=pl.ANY)

    def part_spec(shape, c):
        tail = (0,) * (len(shape) - 1)
        return pl.BlockSpec(shape, lambda i, c=c: (c + i, *tail))

    vec_spec = pl.BlockSpec((1, d, 128), lambda i: (0, 0, vec_at), pipeline_mode=pl.Buffered(1))
    shaped = jax.ShapeDtypeStruct
    names = dict(
        imgs=imgs, groups=groups, gh=gh, gc=gc, hid=hid, prow=prow, trow=trow, tokens=tokens, n_mp=n_mp
    )
    big = (
        shaped((mine * prow, 3 * full), BF16), shaped((mine * prow, d), BF16),
        shaped((mine * wins, groups, WPAD, gh * WPAD), F32), shaped((mine * trow, full), BF16),
    )
    big_fed = (
        shaped((mine * trow, d), F32), shaped((mine * trow, groups * hid), BF16),
        shaped((mine * trow, groups * hid), BF16), shaped((mine * trow, d), BF16),
        shaped((mine * trow, d), BF16),
    )
    probs_block = (imgs * wins, groups, WPAD, gh * WPAD)
    sent, kept, ghbs, sums_bs, arrived = [], [], [], [], []
    first = 0
    for count in (1, steps - 1):
        c = first
        first += count
        relayed = len(sent) > 0
        got_back = pl.pallas_call(
            functools.partial(forward_kernel, kept=len(kept), relayed=relayed, **names),
            out_shape=big + (shaped((count, imgs, tokens, d), BF16),) + big_fed
            + (shaped((groups, 1, hid), F32), shaped((8, d), F32))
            + ((shaped((n_mp,) + sent[0].shape, BF16),) if relayed else ()),
            grid=(count,),
            in_specs=[
                part_spec((imgs, tokens, d), c), part_spec((imgs, tokens, d), c), wa_spec, wb_spec,
                vec_spec, whole(smalls_in.shape), whole(pos.shape), whole(pen.shape), whole(pm.shape),
                whole(pmt.shape),
            ] + [any_spec] * len(kept) + ([whole(sent[0].shape)] if relayed else []),
            out_specs=[
                part_spec((prows, 3 * full), c), part_spec((prows, d), c), part_spec(probs_block, c),
                part_spec((rows, full), c),
                pl.BlockSpec((None, imgs, tokens, d), lambda i: (i, 0, 0, 0)),
                part_spec((rows, d), c), part_spec((rows, groups * hid), c),
                part_spec((rows, groups * hid), c), part_spec((rows, d), c), part_spec((rows, d), c),
                whole((groups, 1, hid)), whole((8, d)),
            ] + ([any_spec] if relayed else []),
            scratch_shapes=[pltpu.VMEM((prows, full), BF16)] + [pltpu.VMEM((rows, d), F32)] * 4
            + (Relay.scratch(sent[0].shape[0], n_mp) if relayed else []),
            input_output_aliases={10 + k: k if k < 4 else k + 1 for k in range(len(kept))},
            compiler_params=pltpu.CompilerParams(
                vmem_limit_bytes=60 * 1024 * 1024,
                **(dict(collective_id=2, has_side_effects=True) if relayed else {}),
            ),
            name="forward",
        )(x_mine, gy_mine, got, got, got, smalls_in, pos, pen, pm, pmt, *kept, *sent)
        kept = list(got_back[0:4]) + list(got_back[5:10])
        sent = [got_back[4]]
        if not relayed:
            sent = [sent[0].reshape(count * imgs, 1, tokens, d)]
        ghbs.append(got_back[10])
        sums_bs.append(got_back[11])
        arrived += [v.reshape(n_mp, -1, imgs, tokens, d) for v in got_back[12:]]
    qkv, hw, probs, attn, gx1, act, gpb, h2, gyp = kept
    gcols = 4 * gc + 2 * hid + 128

    def early(shape):
        tail = (0,) * (len(shape) - 1)
        return pl.BlockSpec(shape, lambda i: (jnp.minimum(i, steps - 1), *tail))

    def late(r, c):
        return pl.BlockSpec((r, c), lambda i: (0, jnp.maximum(i - steps, 0)))

    trows_all, prows_all = mine * trow, mine * prow
    gin, gtab, gqv, gw, out_2 = pl.pallas_call(
        functools.partial(backward_kernel, steps=steps, **names),
        out_shape=(
            shaped((mine, tokens, d), BF16), shaped((groups, WPAD, gh * WPAD), F32),
            shaped((8, full), F32), shaped((groups, d, gcols), BF16),
            shaped((n_mp,) + sent[0].shape, BF16),
        ),
        grid=(steps + groups,),
        in_specs=[
            early((imgs, tokens, d)), early((rows, d)), early((prows, 3 * full)), early(probs_block),
            wa_spec, wp_spec, vec_spec, whole(pmp.shape), whole(pmt.shape), whole(hw.shape),
            whole(gx1.shape), late(trows_all, gc), whole(h2.shape), late(trows_all, hid),
            whole(gyp.shape), late(trows_all, hid), whole((8, d)), whole((8, d)), any_spec,
        ],
        out_specs=[
            early((imgs, tokens, d)), whole((groups, WPAD, gh * WPAD)), whole((8, full)),
            pl.BlockSpec((1, d, gcols), lambda i: (jnp.maximum(i - steps, 0), 0, 0)), any_spec,
        ],
        scratch_shapes=[
            pltpu.VMEM((3, prows_all, full), BF16), pltpu.VMEM((8, d), F32),
            pltpu.VMEM((prows, d), BF16), pltpu.VMEM((prows, full), BF16), pltpu.VMEM((128, d), F32),
            pltpu.VMEM((d, prows_all), BF16), pltpu.VMEM((d, trows_all), BF16),
            pltpu.VMEM((d, trows_all), BF16), pltpu.VMEM((d, trows_all), BF16),
        ] + Relay.scratch(sent[0].shape[0], n_mp),
        compiler_params=pltpu.CompilerParams(
            vmem_limit_bytes=60 * 1024 * 1024, collective_id=3, has_side_effects=True
        ),
        name="backward",
    )(
        x_mine, gx1, qkv, probs, got, got, got, pmp, pmt, hw, gx1, attn, h2, gpb, gyp, act, *sums_bs,
        *sent,
    )
    arrived.append(out_2)
    red, red_s, input_grad = reduce_all(
        gw, rel, gtab, gqv, *ghbs, gin.reshape(steps, imgs, tokens, d), n_dp, n_mp, table_len, gh, gc
    )
    input_grad = input_grad.reshape(images, tokens, d)
    out_parts = arrived
    block_output = jnp.concatenate(out_parts, axis=1).reshape(images, tokens, d)
    gains_t, offs_t, qkv_t, qv_grad, table_grad, proj_grad, fc1_grad, hb_grad, fc2_grad = pl.pallas_call(
        unpack_kernel,
        out_shape=tuple(
            shaped(shape, F32)
            for shape in (
                (2, rows_w), (4, rows_w), (3, rows_w, gc), (2, gc), (gh, table_len), (rows_w, gc),
                (rows_w, hid), (1, hid), (rows_w, hid),
            )
        ),
        name="unpack",
    )(red, red_s)
    return (
        block_output, input_grad, gains_t.T, offs_t.T, qkv_t.transpose(1, 0, 2), qv_grad, table_grad,
        proj_grad, fc1_grad, hb_grad.reshape(hid), fc2_grad,
    )


def solution(mesh):
    in_specs = (
        P("dp", None, None), P("dp", None, None), P("dp", None), P("dp", None), P("dp", None, "mp"),
        P(None, "mp"), P("mp", None), P("dp", "mp"), P("dp", "mp"), P("mp"), P("dp", "mp"), P(), P(),
    )
    out_specs = (
        P("dp", None, None), P("dp", None, None), P("dp", None), P("dp", None), P("dp", None, "mp"),
        P(None, "mp"), P("mp", None), P("dp", "mp"), P("dp", "mp"), P("mp"), P("dp", "mp"),
    )
    body = functools.partial(shards, n_dp=mesh.shape["dp"], n_mp=mesh.shape["mp"])
    return jax.shard_map(body, mesh=mesh, in_specs=in_specs, out_specs=out_specs, check_vma=False)
```
